256 devices in a mesh: shadow: 32 (over z, y_lo, core), vocab: 8 (over y_hi, x).
Axes of the slice: x: 4, y: 4 (y_hi: 2, y_lo: 2; y = y_hi * 2 + y_lo), z: 8, core: 2. Of those that a mesh axis runs over, the one named last changes fastest.
Arguments:
- hidden: bfloat16 [128, 128, 2048], P('shadow'), may hold values from -18 to 18
- targets: int32 [128], replicated, may hold values from 0 to 32767
- membership: int32 [128, 4], P('shadow'), may hold values from 0 to 1, as said below
- unembedding: bfloat16 [32768, 2048], P(('shadow', 'vocab')), may hold values from -1 to 1
Outputs:
- score: float32 [128, 128], P('shadow', 'vocab')
The draws below stay inside these ranges and needn't reach their ends.
Inputs may be any that keep to these rules, and one draw needn't show every extreme that they name: `membership`: each candidate sequence is a member of exactly 64 of the shadow models.
All inputs are finite; a program needn't handle non-finite values.
Results may differ from the reference program's by a relative error of at most 0.00055.
Values may be sent and summed in bfloat16 or wider, within the bound.
A program may use at most 64 MiB of HBM per device.

```python
import math
import jax
import jax.numpy as jnp
import numpy as np
from jax import lax

D = 2048
TOK = 128
SEQ = 32
SHADOWS = 128
VOCAB = 32768
EXAMPLES = 4


def head_table(key):
    unscaled = jax.random.truncated_normal(jax.random.fold_in(key, 11), -4.0, 4.0, (VOCAB, D), jnp.float32)
    return unscaled * D ** (-0.5)


def draw_unembedding(key, part):
    return head_table(key).astype(jnp.bfloat16)


def draw_hidden(key, part):
    states = jnp.clip(jax.random.normal(jax.random.fold_in(key, 12), (SHADOWS, TOK, D), jnp.float32), -4.0, 4.0)
    return states.astype(jnp.bfloat16)


def draw_membership(key, part):
    noise = jax.random.randint(jax.random.fold_in(key, 13), (SHADOWS, EXAMPLES), 0, 1 << 20, jnp.int32)
    noise = noise * SHADOWS + jnp.arange(SHADOWS, dtype=jnp.int32)[:, None]
    ordering = jnp.argsort(noise, axis=0)
    ranking = jnp.argsort(ordering, axis=0)
    return (ranking < SHADOWS // 2).astype(jnp.int32)


def touch_ends(array, own_key, low, high):
    longest = array.shape.index(max(array.shape))
    spots = []
    for shift in (0, 1):
        where = [jax.random.randint(jax.random.fold_in(own_key, axis), (), 0, length) for axis, length in enumerate(array.shape)]
        where[longest] = (where[longest] + shift) % array.shape[longest]
        spots.append(tuple(where))
    return array.at[spots[0]].set(low).at[spots[1]].set(high)


def cumulative_ranks(number_of, lean):
    loads = [(1 << 20) // math.isqrt(standing ** lean) + 1 for standing in range(1, number_of + 1)]
    spread = 1 + sum(loads) // (1 << 30)
    return np.cumsum(np.array([max(1, weight // spread) for weight in loads]))


def skewed_ids(key, shape, amount, skew):
    grid = cumulative_ranks(amount, skew)
    ticket = jax.random.randint(jax.random.fold_in(key, 1), shape, 0, int(grid[amount - 1]))
    rank = jnp.searchsorted(jnp.asarray(grid, jnp.int32), ticket, side="right")
    return jax.random.permutation(jax.random.fold_in(key, 2), amount)[rank].astype(jnp.int32)


def setup_inputs(seed: int = 0) -> dict:
    keys = jax.random.split(jax.random.key(seed), 5)
    hidden = draw_hidden(jax.random.fold_in(keys[4], 71), 0)
    targets = touch_ends(skewed_ids(keys[1], (TOK,), VOCAB, 2), jax.random.fold_in(keys[1], 3), 0, VOCAB - 1).astype(jnp.int32)
    membership = draw_membership(jax.random.fold_in(keys[4], 71), 0)
    unembedding = draw_unembedding(jax.random.fold_in(keys[4], 71), 0)
    return dict(hidden=hidden, targets=targets, membership=membership, unembedding=unembedding)


NEG_FILL = -1e+30
VAR_FLOOR = 0.5

def reference(hidden, targets, membership, unembedding):
    columns = jnp.arange(unembedding.shape[0], dtype=jnp.int32)
    target_hit = targets.astype(jnp.int32)[:, None] == columns[None, :]

    def confidence_of(states):
        logits = lax.dot_general(states, unembedding, (((1,), (1,)), ((), ())), preferred_element_type=jnp.float32)
        target_logit = lax.optimization_barrier(jnp.sum(jnp.where(target_hit, logits, 0.0), axis=1))
        others = jnp.where(target_hit, NEG_FILL, logits)
        highest = lax.optimization_barrier(jnp.max(others, axis=1))
        summed = lax.optimization_barrier(jnp.sum(jnp.where(target_hit, 0.0, jnp.exp(others - highest[:, None])), axis=1))
        return target_logit - (highest + jnp.log(summed))
    confidence = lax.map(confidence_of, hidden)
    outside = (1 - jnp.repeat(membership, SEQ, axis=1)).astype(jnp.float32)
    weighted = outside * confidence
    first_moment = lax.optimization_barrier(jnp.sum(weighted, axis=0))
    second_moment = lax.optimization_barrier(jnp.sum(weighted * confidence, axis=0))
    out_count = SHADOWS // 2 - outside
    out_mean = (first_moment[None, :] - weighted) / out_count
    out_variance = (second_moment[None, :] - weighted * confidence) / out_count - out_mean * out_mean
    return (confidence - out_mean) * lax.rsqrt(jnp.maximum(out_variance, 0.0) + VAR_FLOOR)
```

```python
import functools

import jax
import jax.numpy as jnp
from jax import lax
from jax.experimental import pallas as pl
from jax.experimental.pallas import tpu as pltpu
from jax.sharding import PartitionSpec as P

SEQ = 32
NEG_FILL = -1e30
VAR_FLOOR = 0.5
MESH = pl.DeviceIdType.MESH
NZ = 8
HALF = 64
NT = 256


def kernel(
    hidden_hbm, head_hbm, targets_ref, member_ref, out_ref,
    hid, head, logits, high, total, hit_logit, tg, msg, got1, msg2, got2,
    local_sem, up_send, up_recv, dn_send, dn_recv, yu_send, yu_recv, yd_send, yd_recv,
    core_send, core_recv, tail_send, tail_recv,
):
    shadow = lax.axis_index("shadow")
    vocab = lax.axis_index("vocab")
    z = shadow // 4
    y_lo = (shadow // 2) % 2
    core = shadow % 2
    y_hi = vocab // 4
    x = vocab % 4
    y = y_hi * 2 + y_lo

    def device(z_, y_, x_, core_):
        return ((z_ * 2 + y_ % 2) * 2 + core_, (y_ // 2) * 4 + x_)

    up = device((z + 1) % NZ, y, x, core)
    down = device((z + NZ - 1) % NZ, y, x, core)
    y_up = device(z, (y + 1) % 4, x, core)
    y_dn = device(z, (y + 3) % 4, x, core)
    partner = device(z, y, x, 1 - core)

    own_head = pltpu.make_async_copy(head_hbm, head.at[0], local_sem.at[0])
    own_hid = pltpu.make_async_copy(hidden_hbm, hid.at[0], local_sem.at[1])
    own_head.start()
    own_hid.start()

    place = (y_lo * 2 + core) * 8 + vocab

    def plane_device(p):
        return (z * 4 + p // 8, p % 8)

    barrier = pltpu.get_barrier_semaphore()

    def greet(k, _):
        pl.semaphore_signal(barrier, inc=1, device_id=plane_device((place + k) % 32), device_id_type=MESH)
        return 0

    pl.semaphore_signal(barrier, inc=1, device_id=up, device_id_type=MESH)
    pl.semaphore_signal(barrier, inc=1, device_id=down, device_id_type=MESH)
    lax.fori_loop(1, 32, greet, 0)

    high[...] = jnp.full_like(high, NEG_FILL)
    total[...] = jnp.zeros_like(total)
    hit_logit[...] = jnp.zeros_like(hit_logit)
    wide = jnp.broadcast_to(targets_ref[...], (8, 128))
    tg[:, 0:128] = wide
    tg[:, 128:256] = wide

    pl.semaphore_wait(barrier, 33)
    own_head.wait()

    def ring_copy(k, upward):
        send, recv = (up_send, up_recv) if upward else (dn_send, dn_recv)
        side = 0 if upward else HALF
        if k < 2:
            half = k if upward else 1 - k
            src = head.at[0, pl.ds(half * HALF, HALF), :]
        else:
            src = head.at[k - 1, pl.ds(side, HALF), :]
        return pltpu.make_async_remote_copy(
            src_ref=src, dst_ref=head.at[k + 1, pl.ds(side, HALF), :],
            send_sem=send.at[k], recv_sem=recv.at[k],
            device_id=up if upward else down, device_id_type=MESH,
        )

    for k in range(2):
        ring_copy(k, True).start()
        ring_copy(k, False).start()

    own_hid.wait()

    def y_copy(i, upward):
        send, recv = (yu_send, yu_recv) if upward else (yd_send, yd_recv)
        rows = pl.ds((0 if upward else 256) + i * 128, 128)
        return pltpu.make_async_remote_copy(
            src_ref=hid.at[0, rows, :], dst_ref=hid.at[2, rows, :],
            send_sem=send.at[i], recv_sem=recv.at[i],
            device_id=y_up if upward else y_dn, device_id_type=MESH,
        )

    def core_copy(i):
        if i == 0:
            src, dst = hid.at[0], hid.at[1]
        else:
            rows = pl.ds([0, 256, 128, 384][i - 1], 128)
            src, dst = hid.at[2, rows, :], hid.at[3, rows, :]
        return pltpu.make_async_remote_copy(
            src_ref=src, dst_ref=dst, send_sem=core_send.at[i], recv_sem=core_recv.at[i],
            device_id=partner, device_id_type=MESH,
        )

    for i in range(2):
        y_copy(i, True).start()
        y_copy(i, False).start()
    core_copy(0).start()

    def base_of(u):
        slot, side = u // 2, u % 2
        if slot == 0:
            zs, half = z, side
        else:
            hops = (slot + 1) // 2
            zs = (z + NZ - hops) % NZ if side == 0 else (z + hops) % NZ
            half = (slot + 1) % 2 if side == 0 else slot % 2
        return (((zs * 2 + y_lo) * 2 + core) * 8 + vocab) * 128 + half * HALF

    def product(slot, count, buf, column):
        piece, row = column // 512, pl.multiple_of(column % 512, NT)
        lhs = head[slot:slot + count].reshape(count * 128, head.shape[2])
        rhs = hid[piece, pl.ds(row, NT), :]
        logits[buf, 0:count * 128] = lax.dot_general(
            lhs, rhs, (((1,), (1,)), ((), ())), preferred_element_type=jnp.float32
        )

    def fold(slot, count, buf, column):
        cols = pl.ds(pl.multiple_of(column, NT), NT)
        ids = lax.broadcasted_iota(jnp.int32, (8, 8, NT), 1) + 8 * lax.broadcasted_iota(
            jnp.int32, (8, 8, NT), 0
        )
        found = jnp.zeros((8, NT), jnp.float32)
        others = []
        old = high[:, cols]
        new = old
        for u in range(2 * count):
            v = logits[buf, u * HALF:(u + 1) * HALF, :].reshape(8, 8, NT)
            hit = (tg[...] - base_of(2 * slot + u))[None] == ids
            found = found + jnp.sum(jnp.where(hit, v, 0.0), axis=0)
            v = jnp.where(hit, 2.0 * NEG_FILL, v)
            new = jnp.maximum(new, jnp.max(v, axis=0))
            others.append(v)
        fresh = total[:, cols] * jnp.exp(old - new)
        for v in others:
            fresh = fresh + jnp.sum(jnp.exp(v - new[None]), axis=0)
        high[:, cols] = new
        total[:, cols] = fresh
        hit_logit[:, cols] = hit_logit[:, cols] + found

    def multiply(slot, count, first, columns):
        tiles = columns // NT
        product(slot, count, 0, first)

        def pair(i, _):
            at = first + i * (2 * NT)
            fold(slot, count, 0, at)
            product(slot, count, 1, at + NT)
            fold(slot, count, 1, at + NT)
            product(slot, count, 0, at + 2 * NT)
            return 0

        lax.fori_loop(0, tiles // 2 - 1, pair, 0)
        last = first + columns - 2 * NT
        fold(slot, count, 0, last)
        product(slot, count, 1, last + NT)
        fold(slot, count, 1, last + NT)

    def arrive(k):
        ring_copy(k, True).wait_recv()
        if k < 5:
            ring_copy(k + 2, True).start()
        ring_copy(k, False).wait_recv()
        if k < 5:
            ring_copy(k + 2, False).start()

    def arrive_y(i):
        y_copy(i, True).wait_recv()
        core_copy(1 + 2 * i).start()
        y_copy(i, False).wait_recv()
        core_copy(2 + 2 * i).start()

    core_copy(0).wait_recv()
    arrive(0)
    multiply(0, 2, 0, 1024)
    arrive(1)
    arrive_y(0)
    arrive(2)
    multiply(2, 2, 0, 1024)
    arrive(3)
    arrive_y(1)
    for i in range(1, 5):
        core_copy(i).wait_recv()
    multiply(0, 2, 1024, 1024)
    multiply(2, 2, 1024, 1024)
    arrive(4)
    multiply(4, 2, 0, 2048)
    arrive(5)
    multiply(6, 1, 0, 2048)
    arrive(6)
    multiply(7, 1, 0, 2048)

    lane = lax.broadcasted_iota(jnp.int32, (8, 128), 1)
    line = lax.broadcasted_iota(jnp.int32, (8, 128), 0)
    peak = jnp.max(high[...], axis=0, keepdims=True)
    summed = jnp.sum(total[...] * jnp.exp(high[...] - peak), axis=0, keepdims=True)
    partial = peak + jnp.log(summed)
    at_target = jnp.sum(hit_logit[...], axis=0, keepdims=True)
    for q in range(4):
        tile = jnp.zeros((8, 128), jnp.float32)
        for j in range(4):
            part = slice(q * 512 + j * 128, q * 512 + (j + 1) * 128)
            tile = jnp.where(line == j, jnp.broadcast_to(partial[:, part], (8, 128)), tile)
            tile = jnp.where(line == 4 + j, jnp.broadcast_to(at_target[:, part], (8, 128)), tile)
        swapped = tile
        for d in range(1, 8):
            moved = pltpu.roll(pltpu.roll(tile, d, 0), 128 - 16 * d, 1)
            swapped = jnp.where((line - lane // 16 + 8) % 8 == d, moved, swapped)
        for r in range(8):
            msg[q * 8 + r] = swapped[r:r + 1, :]

    def to_plane(k, _):
        p = (place + k) % 32
        q = ((y_lo + p // 16) % 2) * 2 + (core + p // 8) % 2
        pltpu.make_async_remote_copy(
            src_ref=msg.at[q * 8 + p % 8], dst_ref=got1.at[31 - k],
            send_sem=tail_send.at[0], recv_sem=tail_recv.at[0],
            device_id=plane_device(p), device_id_type=MESH,
        ).start()
        return 0

    lax.fori_loop(1, 32, to_plane, 0)
    got1[31] = msg[vocab]
    all_plane = pltpu.make_async_remote_copy(
        src_ref=msg.at[0:31], dst_ref=got1.at[0:31],
        send_sem=tail_send.at[0], recv_sem=tail_recv.at[0],
        device_id=partner, device_id_type=MESH,
    )
    all_plane.wait_recv()

    lane = lax.broadcasted_iota(jnp.int32, (1, 128), 1)
    pieces = got1[...]
    top = jnp.max(pieces, axis=0)
    lse = top + jnp.log(jnp.sum(jnp.exp(pieces - top[None]), axis=0))
    target_logit = jnp.sum(pieces, axis=0)
    conf = pltpu.roll(target_logit, 64, 1) - lse
    conf = jnp.where(lane < 64, conf, pltpu.roll(conf, 64, 1))
    group = (lane % 64) // 16
    outside = jnp.zeros((1, 128), jnp.float32)
    for j in range(4):
        free = (1 - member_ref[j, vocab // 2]).astype(jnp.float32)
        outside = jnp.where(group == j, free, outside)
    weighted = outside * conf
    squared = weighted * conf

    def over_groups(value):
        value = value + pltpu.roll(value, 16, 1)
        return value + pltpu.roll(value, 32, 1)

    msg2[...] = jnp.where(lane < 64, over_groups(weighted), over_groups(squared))

    def to_shadows(k, _):
        pltpu.make_async_remote_copy(
            src_ref=msg2, dst_ref=got2.at[31 - k],
            send_sem=tail_send.at[1], recv_sem=tail_recv.at[1],
            device_id=((shadow + k) % 32, vocab), device_id_type=MESH,
        ).start()
        return 0

    lax.fori_loop(1, 32, to_shadows, 0)
    got2[31] = msg2[...]
    all_shadows = pltpu.make_async_remote_copy(
        src_ref=got2.at[0:31], dst_ref=got2.at[0:31],
        send_sem=tail_send.at[1], recv_sem=tail_recv.at[1],
        device_id=partner, device_id_type=MESH,
    )
    all_shadows.wait_recv()
    moments = jnp.sum(got2[...], axis=0)
    swapped = pltpu.roll(moments, 64, 1)
    first = jnp.where(lane < 64, moments, swapped)
    second = jnp.where(lane < 64, swapped, moments)
    count = 64.0 - outside
    mean = (first - weighted) / count
    variance = (second - squared) / count - mean * mean
    score = (conf - mean) * lax.rsqrt(jnp.maximum(variance, 0.0) + VAR_FLOOR)
    rows = jnp.broadcast_to(score, (8, 128))
    placed = rows
    for j in range(1, 4):
        placed = jnp.where(line == j, pltpu.roll(rows, 128 - 16 * j, 1), placed)
    out_ref[...] = placed[0:4, 0:16]

    for k in range(7):
        ring_copy(k, True).wait_send()
        ring_copy(k, False).wait_send()
    for i in range(2):
        y_copy(i, True).wait_send()
        y_copy(i, False).wait_send()
    for i in range(5):
        core_copy(i).wait_send()
    all_plane.wait_send()
    all_shadows.wait_send()


def per_device(hidden, targets, membership, unembedding):
    shadow_count, token_count, width = hidden.shape
    return pl.pallas_call(
        kernel,
        out_shape=jax.ShapeDtypeStruct((4, 16), jnp.float32),
        in_specs=[
            pl.BlockSpec(memory_space=pl.ANY),
            pl.BlockSpec(memory_space=pl.ANY),
            pl.BlockSpec(memory_space=pltpu.VMEM),
            pl.BlockSpec(memory_space=pltpu.SMEM),
        ],
        out_specs=pl.BlockSpec(memory_space=pltpu.VMEM),
        scratch_shapes=[
            pltpu.VMEM((4, 512, width), jnp.bfloat16),
            pltpu.VMEM((8, 128, width), jnp.bfloat16),
            pltpu.VMEM((2, 256, NT), jnp.float32),
            pltpu.VMEM((8, 2048), jnp.float32),
            pltpu.VMEM((8, 2048), jnp.float32),
            pltpu.VMEM((8, 2048), jnp.float32),
            pltpu.VMEM((8, NT), jnp.int32),
            pltpu.VMEM((32, 1, 128), jnp.float32),
            pltpu.VMEM((32, 1, 128), jnp.float32),
            pltpu.VMEM((1, 128), jnp.float32),
            pltpu.VMEM((32, 1, 128), jnp.float32),
            pltpu.SemaphoreType.DMA((2,)),
            pltpu.SemaphoreType.DMA((7,)),
            pltpu.SemaphoreType.DMA((7,)),
            pltpu.SemaphoreType.DMA((7,)),
            pltpu.SemaphoreType.DMA((7,)),
            pltpu.SemaphoreType.DMA((2,)),
            pltpu.SemaphoreType.DMA((2,)),
            pltpu.SemaphoreType.DMA((2,)),
            pltpu.SemaphoreType.DMA((2,)),
            pltpu.SemaphoreType.DMA((5,)),
            pltpu.SemaphoreType.DMA((5,)),
            pltpu.SemaphoreType.DMA((2,)),
            pltpu.SemaphoreType.DMA((2,)),
        ],
        compiler_params=pltpu.CompilerParams(
            collective_id=0, has_side_effects=True, vmem_limit_bytes=48 * 2**20
        ),
        name="score_kernel",
    )(
        hidden.reshape(shadow_count * token_count, width), unembedding,
        targets.reshape(1, token_count), membership,
    )


def solution(mesh):
    return jax.shard_map(
        per_device,
        mesh=mesh,
        in_specs=(P("shadow", None, None), P(), P("shadow", None), P(("shadow", "vocab"), None)),
        out_specs=P("shadow", "vocab"),
        check_vma=False,
    )
```

```python
import functools

import jax
import jax.numpy as jnp
from jax import lax
from jax.experimental import pallas as pl
from jax.experimental.pallas import tpu as pltpu
from jax.sharding import PartitionSpec as P

NEG_FILL = -1e30
VAR_FLOOR = 0.5
MESH = pl.DeviceIdType.MESH
NZ = 8
HALF = 64
NT = 256
PARTS = 4
ROWS = 64 // PARTS
CUTS = 2
CUT = HALF // CUTS
FIRST_X = (1, 3, 2)

GROUPS = (
    ((0, 0, 0), (0, 0, 1)),
    ((0, -1, 0), (0, 1, 1)),
    ((-1, 0, 0), (1, 0, 1)),
    ((-1, -1, 0), (1, 1, 1)),
    ((-1, 0, 1), (1, 0, 0)),
    ((1, -1, 0), (-1, 1, 1)),
    ((-2, 0, 0), (2, 0, 1)),
    ((-2, -1, 0), (2, 1, 1)),
)


def kernel(
    hidden_hbm, head_hbm, targets_hbm, member_hbm, out_ref,
    targets_ref, member_ref, bases, hid, head, logits, high, total, hit_logit, tg,
    msg, got1, msg2, got2,
    local_sem, z_send, z_recv, y_send, y_recv, c_send, c_recv,
    hz_send, hz_recv, hy_send, hy_recv, hx_send, hx_recv, tail_send, tail_recv,
):
    shadow = lax.axis_index("shadow")
    vocab = lax.axis_index("vocab")
    z = shadow // 4
    y_lo = (shadow // 2) % 2
    core = shadow % 2
    y_hi = vocab // 4
    x = vocab % 4
    y = y_hi * 2 + y_lo

    def device(dz, dy, dx, dcore):
        to_y = (y + dy) % 4
        return (
            (((z + dz) % NZ) * 2 + to_y % 2) * 2 + (core + dcore) % 2,
            (to_y // 2) * 4 + (x + dx) % 4,
        )

    own_head = pltpu.make_async_copy(head_hbm, head.at[pl.ds(0, 2)], local_sem.at[0])
    own_hid = pltpu.make_async_copy(hidden_hbm, hid.at[0], local_sem.at[1])
    own_tg = pltpu.make_async_copy(targets_hbm, targets_ref, local_sem.at[2])
    own_member = pltpu.make_async_copy(member_hbm, member_ref, local_sem.at[3])
    own_head.start()
    own_hid.start()
    own_tg.start()
    own_member.start()

    barrier = pltpu.get_barrier_semaphore()
    near = ((1, 0, 0, 0), (7, 0, 0, 0), (4, 0, 0, 0), (0, 1, 0, 0), (0, 3, 0, 0), (0, 2, 0, 0), (0, 0, 1, 0), (0, 0, 3, 0), (0, 0, 2, 0), (0, 0, 0, 1))
    for offset in near:
        pl.semaphore_signal(barrier, inc=1, device_id=device(*offset), device_id_type=MESH)

    high[...] = jnp.full_like(high, NEG_FILL)
    total[...] = jnp.zeros_like(total)
    hit_logit[...] = jnp.zeros_like(hit_logit)
    for g in range(8):
        for u in range(4):
            dz, dy, half = GROUPS[g][u % 2]
            at_y = (y + dy + 4) % 4
            block = ((((z + dz + NZ) % NZ) * 2 + at_y % 2) * 2 + (core + u // 2) % 2) * 8 + (at_y // 2) * 4 + x
            bases[4 * g + u] = block * (2 * HALF) + half * HALF
    own_tg.wait()
    own_member.wait()
    wide = jnp.broadcast_to(targets_ref[...], (8, 128))
    tg[:, 0:128] = wide
    tg[:, 128:256] = wide

    def z_copy(k, upward, n):
        rows = pl.ds(n * CUT, CUT)
        side = 0 if upward else 1
        src = (side, 1 - side, 8 + side)[k]
        dst = (8, 16, 24)[k] + side
        return pltpu.make_async_remote_copy(
            src_ref=head.at[src, rows, :], dst_ref=head.at[dst, rows, :],
            send_sem=z_send.at[side, k, n], recv_sem=z_recv.at[side, k, n],
            device_id=device(1 if upward else NZ - 1, 0, 0, 0), device_id_type=MESH,
        )

    def y_copy(m, upward, n):
        rows = pl.ds(n * CUT, CUT)
        side = 0 if upward else 1
        src = ((0, 8, 17, 24) if upward else (1, 9, 16, 25))[m]
        return pltpu.make_async_remote_copy(
            src_ref=head.at[src, rows, :], dst_ref=head.at[8 * m + 4 + side, rows, :],
            send_sem=y_send.at[side, m, n], recv_sem=y_recv.at[side, m, n],
            device_id=device(0, 1 if upward else 3, 0, 0), device_id_type=MESH,
        )

    def c_copy(g, side, n):
        rows = pl.ds(n * CUT, CUT)
        return pltpu.make_async_remote_copy(
            src_ref=head.at[4 * g + side, rows, :], dst_ref=head.at[4 * g + 2 + side, rows, :],
            send_sem=c_send.at[side, g, n], recv_sem=c_recv.at[side, g, n],
            device_id=device(0, 0, 0, 1), device_id_type=MESH,
        )

    def hz_copy(i):
        rows = pl.ds(pl.multiple_of(vocab * 64 + i * ROWS, ROWS), ROWS)
        return pltpu.make_async_remote_copy(
            src_ref=hid.at[0, rows, :], dst_ref=hid.at[1, rows, :],
            send_sem=hz_send.at[i], recv_sem=hz_recv.at[i],
            device_id=device(4, 0, 0, 0), device_id_type=MESH,
        )

    def hy_copy(i):
        rows = pl.ds(pl.multiple_of(vocab * 64 + i * ROWS, ROWS), ROWS)
        return pltpu.make_async_remote_copy(
            src_ref=hid.at[1, rows, :], dst_ref=hid.at[1, rows, :],
            send_sem=hy_send.at[i], recv_sem=hy_recv.at[i],
            device_id=device(0, 2, 0, 0), device_id_type=MESH,
        )

    def hx_copy(part, i, dx):
        owner = x
        to_x = dx
        if len(FIRST_X) == 2 and dx == 2:
            to_x = 1 if i % 2 == 0 else 3
            owner = (x + 4 - to_x) % 4
        share = ((y_hi + part) % 2) * 4 + owner
        rows = pl.ds(pl.multiple_of(share * 64 + i * ROWS, ROWS), ROWS)
        return pltpu.make_async_remote_copy(
            src_ref=hid.at[1, rows, :], dst_ref=hid.at[1, rows, :],
            send_sem=hx_send.at[part, i, dx - 1], recv_sem=hx_recv.at[part, i, dx - 1],
            device_id=device(0, 0, to_x, 0), device_id_type=MESH,
        )

    def product(g, piece, tile):
        lhs = head[pl.ds(4 * g, 4)].reshape(4 * HALF, head.shape[2])
        rhs = hid[piece, tile * NT:(tile + 1) * NT, :]
        logits[tile] = lax.dot_general(
            lhs, rhs, (((1,), (1,)), ((), ())), preferred_element_type=jnp.float32
        )

    def fold(g, piece, tile):
        cols = slice(tile * NT, (tile + 1) * NT)
        ids = lax.broadcasted_iota(jnp.int32, (8, 8, NT), 1) + 8 * lax.broadcasted_iota(
            jnp.int32, (8, 8, NT), 0
        )
        found = hit_logit[piece, :, cols]
        others = []
        old = high[piece, :, cols]
        new = old
        for u in range(4):
            v = logits[tile, u * HALF:(u + 1) * HALF, :].reshape(8, 8, NT)
            hit = (tg[...] - bases[4 * g + u])[None] == ids
            found = found + jnp.sum(jnp.where(hit, v, 0.0), axis=0)
            v = jnp.where(hit, 2.0 * NEG_FILL, v)
            new = jnp.maximum(new, jnp.max(v, axis=0))
            others.append(v)
        fresh = total[piece, :, cols] * jnp.exp(old - new)
        for v in others:
            fresh = fresh + jnp.sum(jnp.exp(v - new[None]), axis=0)
        high[piece, :, cols] = new
        total[piece, :, cols] = fresh
        hit_logit[piece, :, cols] = found

    def multiply(g, piece):
        product(g, piece, 0)
        product(g, piece, 1)
        fold(g, piece, 0)
        fold(g, piece, 1)

    def multiply_many(first, last, piece):
        def step(g, _):
            multiply(g, piece)
            return 0

        lax.fori_loop(first, last, step, 0)

    def on_z(k, n):
        z_copy(k, True, n).wait_recv()
        if k == 0:
            z_copy(2, True, n).start()
        y_copy(k + 1, k != 1, n).start()
        c_copy(2 * k + 2, 0, n).start()
        z_copy(k, False, n).wait_recv()
        if k == 0:
            z_copy(2, False, n).start()
        y_copy(k + 1, k == 1, n).start()
        c_copy(2 * k + 2, 1, n).start()

    def on_y(m, n):
        for side in range(2):
            y_copy(m, side == 0, n).wait_recv()
            c_copy(2 * m + 1, side, n).start()

    def on_c(g):
        for side in range(2):
            for n in range(CUTS):
                c_copy(g, side, n).wait_recv()

    def on_hz(i):
        hz_copy(i).wait_recv()
        hy_copy(i).start()
        for dx in FIRST_X:
            hx_copy(0, i, dx).start()

    def on_hy(i):
        hy_copy(i).wait_recv()
        for dx in FIRST_X:
            hx_copy(1, i, dx).start()

    def on_hx(part, i):
        hx_copy(part, i, 1).wait_recv()
        if i % 2 == 0:
            hx_copy(part, i, 2).start()
        hx_copy(part, i, 3).wait_recv()
        if i % 2 == 1:
            hx_copy(part, i, 2).start()

    def on_hend(first_piece, last_piece):
        for part in range(2):
            for i in range(first_piece, last_piece):
                if len(FIRST_X) == 3:
                    hx_copy(part, i, 1).wait_recv()
                    hx_copy(part, i, 3).wait_recv()
                hx_copy(part, i, 2).wait_recv()

    pl.semaphore_wait(barrier, len(near))
    own_head.wait()
    for n in range(CUTS):
        c_copy(0, 0, n).start()
        c_copy(0, 1, n).start()
    for n in range(CUTS):
        y_copy(0, True, n).start()
        y_copy(0, False, n).start()
    own_hid.wait()
    hz_copy(0).start()
    hz_copy(1).start()
    hz_copy(2).start()
    hz_copy(3).start()
    z_copy(0, True, 0).start()
    z_copy(0, False, 0).start()
    z_copy(0, True, 1).start()
    z_copy(0, False, 1).start()
    z_copy(1, True, 0).start()
    z_copy(1, False, 0).start()
    z_copy(1, True, 1).start()
    z_copy(1, False, 1).start()
    on_c(0)
    multiply(0, 0)
    on_y(0, 0)
    on_hz(0)
    on_y(0, 1)
    on_c(1)
    multiply(1, 0)
    on_hz(1)
    on_hy(0)
    on_hz(2)
    on_hy(1)
    on_hz(3)
    on_z(0, 0)
    on_hy(2)
    on_z(0, 1)
    on_hy(3)
    on_c(2)
    multiply(2, 0)
    on_y(1, 0)
    on_z(1, 0)
    on_y(1, 1)
    on_z(1, 1)
    on_c(3)
    multiply(3, 0)
    on_c(4)
    multiply(4, 0)
    on_y(2, 0)
    on_z(2, 0)
    on_y(2, 1)
    on_z(2, 1)
    on_c(5)
    multiply(5, 0)
    on_c(6)
    multiply(6, 0)
    on_y(3, 0)
    on_hend(0, 4)
    multiply(0, 1)
    multiply(1, 1)
    multiply(2, 1)
    multiply(3, 1)
    on_y(3, 1)
    multiply(4, 1)
    multiply(5, 1)
    multiply(6, 1)
    on_c(7)
    multiply(7, 0)
    multiply(7, 1)

    lane = lax.broadcasted_iota(jnp.int32, (8, 128), 1)
    line = lax.broadcasted_iota(jnp.int32, (8, 128), 0)
    lse_tile = jnp.zeros((8, 128), jnp.float32)
    target_tile = jnp.zeros((8, 128), jnp.float32)
    for piece in range(2):
        peak = jnp.max(high[piece], axis=0, keepdims=True)
        summed = jnp.sum(total[piece] * jnp.exp(high[piece] - peak), axis=0, keepdims=True)
        partial = peak + jnp.log(summed)
        at_target = jnp.sum(hit_logit[piece], axis=0, keepdims=True)
        for j in range(4):
            part = slice(j * 128, (j + 1) * 128)
            here = line == piece * 4 + j
            lse_tile = jnp.where(here, jnp.broadcast_to(partial[:, part], (8, 128)), lse_tile)
            target_tile = jnp.where(here, jnp.broadcast_to(at_target[:, part], (8, 128)), target_tile)

    def swap_groups(tile):
        swapped = tile
        for d in range(1, 8):
            moved = pltpu.roll(pltpu.roll(tile, d, 0), 128 - 16 * d, 1)
            swapped = jnp.where((line - lane // 16 + 8) % 8 == d, moved, swapped)
        return swapped

    lse_tile = swap_groups(lse_tile)
    target_tile = swap_groups(target_tile)
    for r in range(8):
        msg[r, 0] = lse_tile[r:r + 1, :]
        msg[r, 1] = target_tile[r:r + 1, :]

    def to_plane(k, _):
        to = (vocab + k) % 8
        pltpu.make_async_remote_copy(
            src_ref=msg.at[to], dst_ref=got1.at[7 - k],
            send_sem=tail_send.at[0], recv_sem=tail_recv.at[0],
            device_id=(shadow, to), device_id_type=MESH,
        ).start()
        return 0

    lax.fori_loop(1, 8, to_plane, 0)
    got1[7] = msg[vocab]
    all_plane = pltpu.make_async_remote_copy(
        src_ref=msg.at[0:7], dst_ref=got1.at[0:7],
        send_sem=tail_send.at[0], recv_sem=tail_recv.at[0],
        device_id=device(0, 0, 0, 1), device_id_type=MESH,
    )
    lane = lax.broadcasted_iota(jnp.int32, (1, 128), 1)
    group = (lane % 64) // 16
    outside = jnp.zeros((1, 128), jnp.float32)
    for j in range(4):
        free = (1 - member_ref[j, vocab // 2]).astype(jnp.float32)
        outside = jnp.where(group == j, free, outside)
    msg2[2] = outside
    all_plane.wait_recv()

    pieces = got1[:, 0]
    top = jnp.max(pieces, axis=0)
    msg2[0] = top + jnp.log(jnp.sum(jnp.exp(pieces - top[None]), axis=0))
    msg2[1] = jnp.sum(got1[:, 1], axis=0)

    def to_shadows(k, _):
        dz, dy, dcore = k // 4, (k // 2) % 2, k % 2
        to = (((z + dz) % NZ) * 2 + (y_lo + dy) % 2) * 2 + (core + dcore) % 2
        pltpu.make_async_remote_copy(
            src_ref=msg2, dst_ref=got2.at[((NZ - dz) % NZ) * 4 + k % 4],
            send_sem=tail_send.at[1], recv_sem=tail_recv.at[1],
            device_id=(to, vocab), device_id_type=MESH,
        ).start()
        return 0

    lax.fori_loop(1, 32, to_shadows, 0)
    got2[0] = msg2[...]
    all_shadows = pltpu.make_async_remote_copy(
        src_ref=got2.at[1:32], dst_ref=got2.at[1:32],
        send_sem=tail_send.at[1], recv_sem=tail_recv.at[1],
        device_id=device(0, 0, 0, 1), device_id_type=MESH,
    )
    all_shadows.wait_recv()

    def both_planes(row):
        there = jnp.concatenate([got2[16:32, row], got2[0:16, row]], axis=0)
        return got2[:, row], pltpu.roll(there, 64, 2)

    here, there = both_planes(0)
    top = jnp.maximum(here, there)
    lse = top + jnp.log(jnp.exp(here - top) + jnp.exp(there - top))
    here, there = both_planes(1)
    conf = (here + there) - lse
    weighted = jnp.where(lane < 64, got2[:, 2] * conf, 0.0)
    squared = weighted * conf

    def over_groups(value):
        value = jnp.sum(value, axis=0)
        value = value + pltpu.roll(value, 64, 1)
        value = value + pltpu.roll(value, 16, 1)
        return value + pltpu.roll(value, 32, 1)

    first = over_groups(weighted)
    second = over_groups(squared)
    count = 64.0 - outside
    mean = (first - weighted[0]) / count
    variance = (second - squared[0]) / count - mean * mean
    score = (conf[0] - mean) * lax.rsqrt(jnp.maximum(variance, 0.0) + VAR_FLOOR)
    rows = jnp.broadcast_to(score, (8, 128))
    placed = rows
    for j in range(1, 4):
        placed = jnp.where(line == j, pltpu.roll(rows, 128 - 16 * j, 1), placed)
    out_ref[...] = placed[0:4, 0:16]

    for side in range(2):
        for k in range(3):
            for n in range(CUTS):
                z_copy(k, side == 0, n).wait_send()
        for m in range(4):
            for n in range(CUTS):
                y_copy(m, side == 0, n).wait_send()
        for g in range(8):
            for n in range(CUTS):
                c_copy(g, side, n).wait_send()
    for i in range(PARTS):
        hz_copy(i).wait_send()
        hy_copy(i).wait_send()
        for part in range(2):
            for dx in (1, 3, 2):
                hx_copy(part, i, dx).wait_send()
    all_plane.wait_send()
    all_shadows.wait_send()


def per_device(hidden, targets, membership, unembedding):
    shadow_count, token_count, width = hidden.shape
    dma = pltpu.SemaphoreType.DMA
    return pl.pallas_call(
        kernel,
        out_shape=jax.ShapeDtypeStruct((4, 16), jnp.float32),
        in_specs=[pl.BlockSpec(memory_space=pltpu.HBM)] * 4,
        out_specs=pl.BlockSpec(memory_space=pltpu.VMEM),
        scratch_shapes=[
            pltpu.VMEM((1, 128), jnp.int32),
            pltpu.SMEM((4, 4), jnp.int32),
            pltpu.SMEM((32,), jnp.int32),
            pltpu.VMEM((2, 512, width), jnp.bfloat16),
            pltpu.VMEM((32, HALF, width), jnp.bfloat16),
            pltpu.VMEM((2, 4 * HALF, NT), jnp.float32),
            pltpu.VMEM((2, 8, 512), jnp.float32),
            pltpu.VMEM((2, 8, 512), jnp.float32),
            pltpu.VMEM((2, 8, 512), jnp.float32),
            pltpu.VMEM((8, NT), jnp.int32),
            pltpu.VMEM((8, 2, 1, 128), jnp.float32),
            pltpu.VMEM((8, 2, 1, 128), jnp.float32),
            pltpu.VMEM((3, 1, 128), jnp.float32),
            pltpu.VMEM((32, 3, 1, 128), jnp.float32),
            dma((4,)), dma((2, 3, CUTS)), dma((2, 3, CUTS)), dma((2, 4, CUTS)), dma((2, 4, CUTS)),
            dma((2, 8, CUTS)), dma((2, 8, CUTS)),
            dma((PARTS,)), dma((PARTS,)), dma((PARTS,)), dma((PARTS,)),
            dma((2, PARTS, 3)), dma((2, PARTS, 3)), dma((2,)), dma((2,)),
        ],
        compiler_params=pltpu.CompilerParams(
            collective_id=0, has_side_effects=True, vmem_limit_bytes=67043328
        ),
        name="score_kernel",
    )(
        hidden.reshape(shadow_count * token_count, width),
        unembedding.reshape(2, HALF, width),
        targets.reshape(1, token_count), membership,
    )


def solution(mesh):
    return jax.shard_map(
        per_device,
        mesh=mesh,
        in_specs=(P("shadow", None, None), P(), P("shadow", None), P(("shadow", "vocab"), None)),
        out_specs=P("shadow", "vocab"),
        check_vma=False,
    )
```

```python
import functools

import jax
import jax.numpy as jnp
from jax import lax
from jax.experimental import pallas as pl
from jax.experimental.pallas import tpu as pltpu
from jax.sharding import PartitionSpec as P

NEG_FILL = -1e30
VAR_FLOOR = 0.5
MESH = pl.DeviceIdType.MESH
NZ = 8
HALF = 64
NT = 256
PARTS = 4
ROWS = 64 // PARTS
CUTS = 2
CUT = HALF // CUTS
VIA_Z = (1,)
FIRST_X = (1, 3, 2)

GROUPS = (
    ((0, 0, 0), (0, 0, 1)),
    ((0, -1, 0), (0, 1, 1)),
    ((-1, 0, 0), (1, 0, 1)),
    ((-1, -1, 0), (1, 1, 1)),
    ((-1, 0, 1), (1, 0, 0)),
    ((1, -1, 0), (-1, 1, 1)),
    ((-2, 0, 0), (2, 0, 1)),
    ((-2, -1, 0), (2, 1, 1)),
)


def kernel(
    hidden_hbm, head_hbm, targets_hbm, member_hbm, out_ref,
    targets_ref, member_ref, bases, hid, head, logits, high, total, hit_logit, tg,
    msg, got1, msg2, got2,
    local_sem, z_send, z_recv, y_send, y_recv, c_send, c_recv,
    hz_send, hz_recv, hy_send, hy_recv, hx_send, hx_recv, tail_send, tail_recv,
):
    shadow = lax.axis_index("shadow")
    vocab = lax.axis_index("vocab")
    z = shadow // 4
    y_lo = (shadow // 2) % 2
    core = shadow % 2
    y_hi = vocab // 4
    x = vocab % 4
    y = y_hi * 2 + y_lo

    def device(dz, dy, dx, dcore):
        to_y = (y + dy) % 4
        return (
            (((z + dz) % NZ) * 2 + to_y % 2) * 2 + (core + dcore) % 2,
            (to_y // 2) * 4 + (x + dx) % 4,
        )

    own_head = pltpu.make_async_copy(head_hbm, head.at[pl.ds(0, 2)], local_sem.at[0])
    own_hid = pltpu.make_async_copy(hidden_hbm, hid.at[0], local_sem.at[1])
    own_tg = pltpu.make_async_copy(targets_hbm, targets_ref, local_sem.at[2])
    own_member = pltpu.make_async_copy(member_hbm, member_ref, local_sem.at[3])
    own_head.start()
    own_hid.start()
    own_tg.start()
    own_member.start()

    barrier = pltpu.get_barrier_semaphore()
    near = ((1, 0, 0, 0), (7, 0, 0, 0), (4, 0, 0, 0), (0, 1, 0, 0), (0, 3, 0, 0), (0, 2, 0, 0), (0, 0, 1, 0), (0, 0, 3, 0), (0, 0, 2, 0), (0, 0, 0, 1))
    for offset in near:
        pl.semaphore_signal(barrier, inc=1, device_id=device(*offset), device_id_type=MESH)

    high[...] = jnp.full_like(high, NEG_FILL)
    total[...] = jnp.zeros_like(total)
    hit_logit[...] = jnp.zeros_like(hit_logit)
    for g in range(8):
        for u in range(4):
            dz, dy, half = GROUPS[g][u % 2]
            at_y = (y + dy + 4) % 4
            block = ((((z + dz + NZ) % NZ) * 2 + at_y % 2) * 2 + (core + u // 2) % 2) * 8 + (at_y // 2) * 4 + x
            bases[4 * g + u] = block * (2 * HALF) + half * HALF
    own_tg.wait()
    own_member.wait()
    wide = jnp.broadcast_to(targets_ref[...], (8, 128))
    tg[:, 0:128] = wide
    tg[:, 128:256] = wide

    def z_copy(k, upward, n):
        rows = pl.ds(n * CUT, CUT)
        side = 0 if upward else 1
        src = (side, 1 - side, 8 + side, 12 + side)[k]
        dst = (8, 16, 24, 28)[k] + side
        return pltpu.make_async_remote_copy(
            src_ref=head.at[src, rows, :], dst_ref=head.at[dst, rows, :],
            send_sem=z_send.at[side, k, n], recv_sem=z_recv.at[side, k, n],
            device_id=device(1 if upward else NZ - 1, 0, 0, 0), device_id_type=MESH,
        )

    def y_copy(m, upward, n):
        rows = pl.ds(n * CUT, CUT)
        side = 0 if upward else 1
        src = ((0, 8, 17, 24) if upward else (1, 9, 16, 25))[m]
        return pltpu.make_async_remote_copy(
            src_ref=head.at[src, rows, :], dst_ref=head.at[8 * m + 4 + side, rows, :],
            send_sem=y_send.at[side, m, n], recv_sem=y_recv.at[side, m, n],
            device_id=device(0, 1 if upward else 3, 0, 0), device_id_type=MESH,
        )

    def c_copy(g, side, n):
        rows = pl.ds(n * CUT, CUT)
        return pltpu.make_async_remote_copy(
            src_ref=head.at[4 * g + side, rows, :], dst_ref=head.at[4 * g + 2 + side, rows, :],
            send_sem=c_send.at[side, g, n], recv_sem=c_recv.at[side, g, n],
            device_id=device(0, 0, 0, 1), device_id_type=MESH,
        )

    def hz_copy(i):
        rows = pl.ds(pl.multiple_of(vocab * 64 + i * ROWS, ROWS), ROWS)
        return pltpu.make_async_remote_copy(
            src_ref=hid.at[0, rows, :], dst_ref=hid.at[1, rows, :],
            send_sem=hz_send.at[i], recv_sem=hz_recv.at[i],
            device_id=device(4, 0, 0, 0), device_id_type=MESH,
        )

    def hy_copy(i):
        rows = pl.ds(pl.multiple_of(vocab * 64 + i * ROWS, ROWS), ROWS)
        return pltpu.make_async_remote_copy(
            src_ref=hid.at[1, rows, :], dst_ref=hid.at[1, rows, :],
            send_sem=hy_send.at[i], recv_sem=hy_recv.at[i],
            device_id=device(0, 2, 0, 0), device_id_type=MESH,
        )

    def hx_copy(part, i, dx):
        share = ((y_hi + part) % 2) * 4 + x
        rows = pl.ds(pl.multiple_of(share * 64 + i * ROWS, ROWS), ROWS)
        return pltpu.make_async_remote_copy(
            src_ref=hid.at[1, rows, :], dst_ref=hid.at[1, rows, :],
            send_sem=hx_send.at[part, i, dx - 1], recv_sem=hx_recv.at[part, i, dx - 1],
            device_id=device(0, 0, dx, 0), device_id_type=MESH,
        )

    def columns(tile):
        return pl.ds(pl.multiple_of(tile * NT, NT), NT)

    def product(g, count, piece, tile, buf):
        lhs = head[4 * g:4 * (g + count)].reshape(4 * count * HALF, head.shape[2])
        rhs = hid[piece, columns(tile), :]
        logits[buf, 0:4 * count * HALF] = lax.dot_general(
            lhs, rhs, (((1,), (1,)), ((), ())), preferred_element_type=jnp.float32
        )

    def fold(first, count, piece, tile, buf):
        for g in range(first, first + count):
            fold_group(g, (g - first) * 4, piece, columns(tile), buf)

    def fold_group(g, at, piece, cols, buf):
        ids = lax.broadcasted_iota(jnp.int32, (8, 8, NT), 1) + 8 * lax.broadcasted_iota(
            jnp.int32, (8, 8, NT), 0
        )
        found = hit_logit[piece, :, cols]
        others = []
        old = high[piece, :, cols]
        new = old
        for u in range(4):
            v = logits[buf, (at + u) * HALF:(at + u + 1) * HALF, :].reshape(8, 8, NT)
            hit = (tg[...] - bases[4 * g + u])[None] == ids
            found = found + jnp.sum(jnp.where(hit, v, 0.0), axis=0)
            v = jnp.where(hit, 2.0 * NEG_FILL, v)
            new = jnp.maximum(new, jnp.max(v, axis=0))
            others.append(v)
        fresh = total[piece, :, cols] * jnp.exp(old - new)
        for v in others:
            fresh = fresh + jnp.sum(jnp.exp(v - new[None]), axis=0)
        high[piece, :, cols] = new
        total[piece, :, cols] = fresh
        hit_logit[piece, :, cols] = found

    def multiply(*tiles):
        for i, tile in enumerate(tiles):
            product(*tile, i % 4)
            if i:
                fold(*tiles[i - 1], (i - 1) % 4)
        fold(*tiles[-1], (len(tiles) - 1) % 4)

    own_tile, far_tile = y_hi, 1 - y_hi

    def on_z(k, n):
        for side in range(2):
            upward = side == 0
            z_copy(k, upward, n).wait_recv()
            if k == 0:
                z_copy(2, upward, n).start()
            if k < 2 or (k == 2 and n not in VIA_Z):
                y_copy(k + 1, upward == (k != 1), n).start()
            c_copy(7 if k == 3 else 2 * k + 2, side, n).start()

    def on_y(m, n):
        for side in range(2):
            y_copy(m, side == 0, n).wait_recv()
            if m == 1 and n in VIA_Z:
                z_copy(3, side == 0, n).start()
            c_copy(2 * m + 1, side, n).start()

    def on_c(g):
        for side in range(2):
            for n in range(CUTS):
                c_copy(g, side, n).wait_recv()

    def on_hz(i):
        hz_copy(i).wait_recv()
        hy_copy(i).start()
        for dx in FIRST_X:
            hx_copy(0, i, dx).start()

    def on_hy(i):
        hy_copy(i).wait_recv()
        for dx in FIRST_X:
            hx_copy(1, i, dx).start()

    def on_hend(part):
        for i in range(PARTS):
            for dx in (1, 3, 2):
                hx_copy(part, i, dx).wait_recv()

    pl.semaphore_wait(barrier, len(near))
    own_head.wait()
    for n in range(CUTS):
        c_copy(0, 0, n).start()
        c_copy(0, 1, n).start()
    for n in range(CUTS):
        y_copy(0, True, n).start()
        y_copy(0, False, n).start()
    own_hid.wait()
    hz_copy(0).start()
    hz_copy(1).start()
    hz_copy(2).start()
    hz_copy(3).start()
    z_copy(0, True, 0).start()
    z_copy(0, False, 0).start()
    z_copy(0, True, 1).start()
    z_copy(0, False, 1).start()
    z_copy(1, True, 0).start()
    z_copy(1, False, 0).start()
    z_copy(1, True, 1).start()
    z_copy(1, False, 1).start()
    on_c(0)
    multiply((0, 1, 0, 0), (0, 1, 0, 1))
    on_y(0, 0)
    on_hz(0)
    on_y(0, 1)
    on_c(1)
    multiply((1, 1, 0, 0), (1, 1, 0, 1))
    on_hz(1)
    on_hy(0)
    on_hz(2)
    on_hy(1)
    on_hz(3)
    on_z(0, 0)
    on_hy(2)
    on_z(0, 1)
    on_hy(3)
    on_c(2)
    multiply((2, 1, 0, 0), (2, 1, 0, 1))
    on_y(1, 0)
    on_z(1, 0)
    on_y(1, 1)
    on_z(1, 1)
    on_c(3)
    on_c(4)
    multiply((3, 1, 0, 0), (3, 1, 0, 1), (4, 1, 0, 0), (4, 1, 0, 1))
    on_y(2, 0)
    on_z(2, 0)
    on_hend(0)
    multiply((0, 1, 1, own_tile), (1, 1, 1, own_tile), (2, 1, 1, own_tile), (3, 1, 1, own_tile))
    on_y(2, 1)
    on_z(2, 1)
    multiply((4, 1, 1, own_tile))
    on_c(5)
    on_c(6)
    multiply((5, 1, 0, 0), (5, 1, 0, 1), (6, 1, 0, 0), (6, 1, 0, 1))
    on_y(3, 0)
    on_z(3, 1)
    multiply((5, 1, 1, own_tile), (6, 1, 1, own_tile))
    on_hend(1)
    multiply((0, 1, 1, far_tile), (1, 1, 1, far_tile), (2, 1, 1, far_tile), (3, 1, 1, far_tile), (4, 1, 1, far_tile), (5, 1, 1, far_tile), (6, 1, 1, far_tile))
    on_c(7)
    multiply((7, 1, 0, 0), (7, 1, 0, 1), (7, 1, 1, own_tile), (7, 1, 1, far_tile))

    lane = lax.broadcasted_iota(jnp.int32, (8, 128), 1)
    line = lax.broadcasted_iota(jnp.int32, (8, 128), 0)
    lse_tile = jnp.zeros((8, 128), jnp.float32)
    target_tile = jnp.zeros((8, 128), jnp.float32)
    for piece in range(2):
        peak = jnp.max(high[piece], axis=0, keepdims=True)
        summed = jnp.sum(total[piece] * jnp.exp(high[piece] - peak), axis=0, keepdims=True)
        partial = peak + jnp.log(summed)
        at_target = jnp.sum(hit_logit[piece], axis=0, keepdims=True)
        for j in range(4):
            part = slice(j * 128, (j + 1) * 128)
            here = line == piece * 4 + j
            lse_tile = jnp.where(here, jnp.broadcast_to(partial[:, part], (8, 128)), lse_tile)
            target_tile = jnp.where(here, jnp.broadcast_to(at_target[:, part], (8, 128)), target_tile)

    def swap_groups(tile):
        swapped = tile
        for d in range(1, 8):
            moved = pltpu.roll(pltpu.roll(tile, d, 0), 128 - 16 * d, 1)
            swapped = jnp.where((line - lane // 16 + 8) % 8 == d, moved, swapped)
        return swapped

    lse_tile = swap_groups(lse_tile)
    target_tile = swap_groups(target_tile)
    for r in range(8):
        msg[r, 0] = lse_tile[r:r + 1, :]
        msg[r, 1] = target_tile[r:r + 1, :]

    def to_plane(k, _):
        to = (vocab + k) % 8
        pltpu.make_async_remote_copy(
            src_ref=msg.at[to], dst_ref=got1.at[7 - k],
            send_sem=tail_send.at[0], recv_sem=tail_recv.at[0],
            device_id=(shadow, to), device_id_type=MESH,
        ).start()
        return 0

    lax.fori_loop(1, 8, to_plane, 0)
    got1[7] = msg[vocab]
    all_plane = pltpu.make_async_remote_copy(
        src_ref=msg.at[0:7], dst_ref=got1.at[0:7],
        send_sem=tail_send.at[0], recv_sem=tail_recv.at[0],
        device_id=device(0, 0, 0, 1), device_id_type=MESH,
    )
    lane = lax.broadcasted_iota(jnp.int32, (1, 128), 1)
    group = (lane % 64) // 16
    outside = jnp.zeros((1, 128), jnp.float32)
    for j in range(4):
        free = (1 - member_ref[j, vocab // 2]).astype(jnp.float32)
        outside = jnp.where(group == j, free, outside)
    msg2[2] = outside
    all_plane.wait_recv()

    pieces = got1[:, 0]
    top = jnp.max(pieces, axis=0)
    msg2[0] = top + jnp.log(jnp.sum(jnp.exp(pieces - top[None]), axis=0))
    msg2[1] = jnp.sum(got1[:, 1], axis=0)

    def to_shadows(k, _):
        dz, dy, dcore = k // 4, (k // 2) % 2, k % 2
        to = (((z + dz) % NZ) * 2 + (y_lo + dy) % 2) * 2 + (core + dcore) % 2
        pltpu.make_async_remote_copy(
            src_ref=msg2, dst_ref=got2.at[((NZ - dz) % NZ) * 4 + k % 4],
            send_sem=tail_send.at[1], recv_sem=tail_recv.at[1],
            device_id=(to, vocab), device_id_type=MESH,
        ).start()
        return 0

    lax.fori_loop(1, 32, to_shadows, 0)
    got2[0] = msg2[...]
    all_shadows = pltpu.make_async_remote_copy(
        src_ref=got2.at[1:32], dst_ref=got2.at[1:32],
        send_sem=tail_send.at[1], recv_sem=tail_recv.at[1],
        device_id=device(0, 0, 0, 1), device_id_type=MESH,
    )
    all_shadows.wait_recv()

    def both_planes(row):
        there = jnp.concatenate([got2[16:32, row], got2[0:16, row]], axis=0)
        return got2[:, row], pltpu.roll(there, 64, 2)

    here, there = both_planes(0)
    top = jnp.maximum(here, there)
    lse = top + jnp.log(jnp.exp(here - top) + jnp.exp(there - top))
    here, there = both_planes(1)
    conf = (here + there) - lse
    weighted = jnp.where(lane < 64, got2[:, 2] * conf, 0.0)
    squared = weighted * conf

    def over_groups(value):
        value = jnp.sum(value, axis=0)
        value = value + pltpu.roll(value, 64, 1)
        value = value + pltpu.roll(value, 16, 1)
        return value + pltpu.roll(value, 32, 1)

    first = over_groups(weighted)
    second = over_groups(squared)
    count = 64.0 - outside
    mean = (first - weighted[0]) / count
    variance = (second - squared[0]) / count - mean * mean
    score = (conf[0] - mean) * lax.rsqrt(jnp.maximum(variance, 0.0) + VAR_FLOOR)
    rows = jnp.broadcast_to(score, (8, 128))
    placed = rows
    for j in range(1, 4):
        placed = jnp.where(line == j, pltpu.roll(rows, 128 - 16 * j, 1), placed)
    out_ref[...] = placed[0:4, 0:16]

    for side in range(2):
        for k in range(4):
            for n in VIA_Z if k == 3 else range(CUTS):
                z_copy(k, side == 0, n).wait_send()
        for m in range(4):
            for n in range(CUTS):
                if m < 3 or n not in VIA_Z:
                    y_copy(m, side == 0, n).wait_send()
        for g in range(8):
            for n in range(CUTS):
                c_copy(g, side, n).wait_send()
    for i in range(PARTS):
        hz_copy(i).wait_send()
        hy_copy(i).wait_send()
        for part in range(2):
            for dx in (1, 3, 2):
                hx_copy(part, i, dx).wait_send()
    all_plane.wait_send()
    all_shadows.wait_send()


def per_device(hidden, targets, membership, unembedding):
    shadow_count, token_count, width = hidden.shape
    dma = pltpu.SemaphoreType.DMA
    return pl.pallas_call(
        kernel,
        out_shape=jax.ShapeDtypeStruct((4, 16), jnp.float32),
        in_specs=[pl.BlockSpec(memory_space=pltpu.HBM)] * 4,
        out_specs=pl.BlockSpec(memory_space=pltpu.VMEM),
        scratch_shapes=[
            pltpu.VMEM((1, 128), jnp.int32),
            pltpu.SMEM((4, 4), jnp.int32),
            pltpu.SMEM((32,), jnp.int32),
            pltpu.VMEM((2, 512, width), jnp.bfloat16),
            pltpu.VMEM((32, HALF, width), jnp.bfloat16),
            pltpu.VMEM((4, 8 * HALF, NT), jnp.float32),
            pltpu.VMEM((2, 8, 512), jnp.float32),
            pltpu.VMEM((2, 8, 512), jnp.float32),
            pltpu.VMEM((2, 8, 512), jnp.float32),
            pltpu.VMEM((8, NT), jnp.int32),
            pltpu.VMEM((8, 2, 1, 128), jnp.float32),
            pltpu.VMEM((8, 2, 1, 128), jnp.float32),
            pltpu.VMEM((3, 1, 128), jnp.float32),
            pltpu.VMEM((32, 3, 1, 128), jnp.float32),
            dma((4,)), dma((2, 4, CUTS)), dma((2, 4, CUTS)), dma((2, 4, CUTS)), dma((2, 4, CUTS)),
            dma((2, 8, CUTS)), dma((2, 8, CUTS)),
            dma((PARTS,)), dma((PARTS,)), dma((PARTS,)), dma((PARTS,)),
            dma((2, PARTS, 3)), dma((2, PARTS, 3)), dma((2,)), dma((2,)),
        ],
        compiler_params=pltpu.CompilerParams(
            collective_id=0, has_side_effects=True, vmem_limit_bytes=67043328
        ),
        name="score_kernel",
    )(
        hidden.reshape(shadow_count * token_count, width),
        unembedding.reshape(2, HALF, width),
        targets.reshape(1, token_count), membership,
    )


def solution(mesh):
    return jax.shard_map(
        per_device,
        mesh=mesh,
        in_specs=(P("shadow", None, None), P(), P("shadow", None), P(("shadow", "vocab"), None)),
        out_specs=P("shadow", "vocab"),
        check_vma=False,
    )
```

```python
import functools

import jax
import jax.numpy as jnp
from jax import lax
from jax.experimental import pallas as pl
from jax.experimental.pallas import tpu as pltpu
from jax.sharding import PartitionSpec as P

NEG_FILL = -1e30
VAR_FLOOR = 0.5
MESH = pl.DeviceIdType.MESH
NZ = 8
HALF = 64
NT = 256
PARTS = 4
ROWS = 64 // PARTS
CUTS = 2
CUT = HALF // CUTS
VIA_Z = (1,)
FIRST_X = (1, 3, 2)

GROUPS = (
    ((0, 0, 0), (0, 0, 1)),
    ((0, -1, 0), (0, 1, 1)),
    ((-1, 0, 0), (1, 0, 1)),
    ((-1, -1, 0), (1, 1, 1)),
    ((-1, 0, 1), (1, 0, 0)),
    ((1, -1, 0), (-1, 1, 1)),
    ((-2, 0, 0), (2, 0, 1)),
    ((-2, -1, 0), (2, 1, 1)),
)


def kernel(
    hidden_hbm, head_hbm, targets_hbm, member_hbm, out_ref,
    targets_ref, member_ref, bases, hid, head, logits, high, total, hit_logit, tg,
    msg, got1, msg2, got2,
    local_sem, z_send, z_recv, y_send, y_recv, c_send, c_recv,
    hz_send, hz_recv, hy_send, hy_recv, hx_send, hx_recv, tail_send, tail_recv,
):
    shadow = lax.axis_index("shadow")
    vocab = lax.axis_index("vocab")
    z = shadow // 4
    y_lo = (shadow // 2) % 2
    core = shadow % 2
    y_hi = vocab // 4
    x = vocab % 4
    y = y_hi * 2 + y_lo

    def device(dz, dy, dx, dcore):
        to_y = (y + dy) % 4
        return (
            (((z + dz) % NZ) * 2 + to_y % 2) * 2 + (core + dcore) % 2,
            (to_y // 2) * 4 + (x + dx) % 4,
        )

    own_head = pltpu.make_async_copy(head_hbm, head.at[pl.ds(0, 2)], local_sem.at[0])
    own_hid = pltpu.make_async_copy(hidden_hbm, hid.at[0], local_sem.at[1])
    own_tg = pltpu.make_async_copy(targets_hbm, targets_ref, local_sem.at[2])
    own_member = pltpu.make_async_copy(member_hbm, member_ref, local_sem.at[3])
    own_head.start()
    own_hid.start()
    own_tg.start()
    own_member.start()

    barrier = pltpu.get_barrier_semaphore()
    near = ((1, 0, 0, 0), (7, 0, 0, 0), (4, 0, 0, 0), (0, 1, 0, 0), (0, 3, 0, 0), (0, 2, 0, 0), (0, 0, 1, 0), (0, 0, 3, 0), (0, 0, 2, 0), (0, 0, 0, 1))
    for offset in near:
        pl.semaphore_signal(barrier, inc=1, device_id=device(*offset), device_id_type=MESH)

    high[...] = jnp.full_like(high, NEG_FILL)
    total[...] = jnp.zeros_like(total)
    hit_logit[...] = jnp.zeros_like(hit_logit)
    for g in range(8):
        for u in range(4):
            dz, dy, half = GROUPS[g][u % 2]
            at_y = (y + dy + 4) % 4
            block = ((((z + dz + NZ) % NZ) * 2 + at_y % 2) * 2 + (core + u // 2) % 2) * 8 + (at_y // 2) * 4 + x
            bases[4 * g + u] = block * (2 * HALF) + half * HALF
    own_tg.wait()
    own_member.wait()
    wide = jnp.broadcast_to(targets_ref[...], (8, 128))
    tg[:, 0:128] = wide
    tg[:, 128:256] = wide

    def z_copy(k, upward, n):
        rows = pl.ds(n * CUT, CUT)
        side = 0 if upward else 1
        src = (side, 1 - side, 8 + side, 12 + side)[k]
        dst = (8, 16, 24, 28)[k] + side
        return pltpu.make_async_remote_copy(
            src_ref=head.at[src, rows, :], dst_ref=head.at[dst, rows, :],
            send_sem=z_send.at[side, k, n], recv_sem=z_recv.at[side, k, n],
            device_id=device(1 if upward else NZ - 1, 0, 0, 0), device_id_type=MESH,
        )

    def y_copy(m, upward, n):
        rows = pl.ds(n * CUT, CUT)
        side = 0 if upward else 1
        src = ((0, 8, 17, 24) if upward else (1, 9, 16, 25))[m]
        return pltpu.make_async_remote_copy(
            src_ref=head.at[src, rows, :], dst_ref=head.at[8 * m + 4 + side, rows, :],
            send_sem=y_send.at[side, m, n], recv_sem=y_recv.at[side, m, n],
            device_id=device(0, 1 if upward else 3, 0, 0), device_id_type=MESH,
        )

    def c_copy(g, side, n):
        rows = pl.ds(n * CUT, CUT)
        return pltpu.make_async_remote_copy(
            src_ref=head.at[4 * g + side, rows, :], dst_ref=head.at[4 * g + 2 + side, rows, :],
            send_sem=c_send.at[side, g, n], recv_sem=c_recv.at[side, g, n],
            device_id=device(0, 0, 0, 1), device_id_type=MESH,
        )

    def hz_copy(i):
        rows = pl.ds(pl.multiple_of(vocab * 64 + i * ROWS, ROWS), ROWS)
        return pltpu.make_async_remote_copy(
            src_ref=hid.at[0, rows, :], dst_ref=hid.at[1, rows, :],
            send_sem=hz_send.at[i], recv_sem=hz_recv.at[i],
            device_id=device(4, 0, 0, 0), device_id_type=MESH,
        )

    def hy_copy(i):
        rows = pl.ds(pl.multiple_of(vocab * 64 + i * ROWS, ROWS), ROWS)
        return pltpu.make_async_remote_copy(
            src_ref=hid.at[1, rows, :], dst_ref=hid.at[1, rows, :],
            send_sem=hy_send.at[i], recv_sem=hy_recv.at[i],
            device_id=device(0, 2, 0, 0), device_id_type=MESH,
        )

    def hx_copy(part, i, dx):
        to_x, owner = dx, x
        if part == 1 and dx == 2:
            to_x = 1 if i % 2 == 0 else 3
            owner = (x + 4 - to_x) % 4
        share = ((y_hi + part) % 2) * 4 + owner
        rows = pl.ds(pl.multiple_of(share * 64 + i * ROWS, ROWS), ROWS)
        return pltpu.make_async_remote_copy(
            src_ref=hid.at[1, rows, :], dst_ref=hid.at[1, rows, :],
            send_sem=hx_send.at[part, i, dx - 1], recv_sem=hx_recv.at[part, i, dx - 1],
            device_id=device(0, 0, to_x, 0), device_id_type=MESH,
        )

    def columns(tile):
        return pl.ds(pl.multiple_of(tile * NT, NT), NT)

    def product(g, count, piece, tile, buf):
        lhs = head[4 * g:4 * (g + count)].reshape(4 * count * HALF, head.shape[2])
        rhs = hid[piece, columns(tile), :]
        logits[buf, 0:4 * count * HALF] = lax.dot_general(
            lhs, rhs, (((1,), (1,)), ((), ())), preferred_element_type=jnp.float32
        )

    def fold(first, count, piece, tile, buf):
        for g in range(first, first + count):
            fold_group(g, (g - first) * 4, piece, columns(tile), buf)

    def fold_group(g, at, piece, cols, buf):
        ids = lax.broadcasted_iota(jnp.int32, (8, 8, NT), 1) + 8 * lax.broadcasted_iota(
            jnp.int32, (8, 8, NT), 0
        )
        found = hit_logit[piece, :, cols]
        others = []
        old = high[piece, :, cols]
        new = old
        for u in range(4):
            v = logits[buf, (at + u) * HALF:(at + u + 1) * HALF, :].reshape(8, 8, NT)
            hit = (tg[...] - bases[4 * g + u])[None] == ids
            found = found + jnp.sum(jnp.where(hit, v, 0.0), axis=0)
            v = jnp.where(hit, 2.0 * NEG_FILL, v)
            new = jnp.maximum(new, jnp.max(v, axis=0))
            others.append(v)
        fresh = total[piece, :, cols] * jnp.exp(old - new)
        for v in others:
            fresh = fresh + jnp.sum(jnp.exp(v - new[None]), axis=0)
        high[piece, :, cols] = new
        total[piece, :, cols] = fresh
        hit_logit[piece, :, cols] = found

    def multiply(*tiles):
        for i, tile in enumerate(tiles):
            product(*tile, i % 4)
            if i:
                fold(*tiles[i - 1], (i - 1) % 4)
        fold(*tiles[-1], (len(tiles) - 1) % 4)

    own_tile, far_tile = y_hi, 1 - y_hi

    def on_z(k, n):
        for side in range(2):
            upward = side == 0
            z_copy(k, upward, n).wait_recv()
            if k == 0:
                z_copy(2, upward, n).start()
            if k < 2 or (k == 2 and n not in VIA_Z):
                y_copy(k + 1, upward == (k != 1), n).start()
            c_copy(7 if k == 3 else 2 * k + 2, side, n).start()

    def on_y(m, n):
        for side in range(2):
            y_copy(m, side == 0, n).wait_recv()
            if m == 1 and n in VIA_Z:
                z_copy(3, side == 0, n).start()
            c_copy(2 * m + 1, side, n).start()

    def on_c(g):
        for side in range(2):
            for n in range(CUTS):
                c_copy(g, side, n).wait_recv()

    def on_hz(i):
        hz_copy(i).wait_recv()
        hy_copy(i).start()
        for dx in FIRST_X:
            hx_copy(0, i, dx).start()

    def on_hy(i):
        hy_copy(i).wait_recv()
        for dx in (1, 3):
            hx_copy(1, i, dx).start()

    def on_hx(i):
        for dx in (1, 3):
            hx_copy(1, i, dx).wait_recv()
            if (dx == 1) == (i % 2 == 0):
                hx_copy(1, i, 2).start()

    def on_hend(part):
        for i in range(PARTS):
            for dx in (1, 3, 2) if part == 0 else (2,):
                hx_copy(part, i, dx).wait_recv()

    pl.semaphore_wait(barrier, len(near))
    own_head.wait()
    for n in range(CUTS):
        c_copy(0, 0, n).start()
        c_copy(0, 1, n).start()
    for n in range(CUTS):
        y_copy(0, True, n).start()
        y_copy(0, False, n).start()
    own_hid.wait()
    hz_copy(0).start()
    hz_copy(1).start()
    hz_copy(2).start()
    hz_copy(3).start()
    z_copy(0, True, 0).start()
    z_copy(0, False, 0).start()
    z_copy(0, True, 1).start()
    z_copy(0, False, 1).start()
    z_copy(1, True, 0).start()
    z_copy(1, False, 0).start()
    z_copy(1, True, 1).start()
    z_copy(1, False, 1).start()
    on_c(0)
    multiply((0, 1, 0, 0), (0, 1, 0, 1))
    on_y(0, 0)
    on_hz(0)
    on_y(0, 1)
    on_c(1)
    multiply((1, 1, 0, 0), (1, 1, 0, 1))
    on_hz(1)
    on_hz(2)
    on_hz(3)
    on_hy(0)
    on_hy(1)
    on_z(0, 0)
    on_hy(2)
    on_z(0, 1)
    on_hy(3)
    on_c(2)
    multiply((2, 1, 0, 0), (2, 1, 0, 1))
    on_y(1, 0)
    on_z(1, 0)
    on_hx(0)
    on_hx(1)
    on_hend(0)
    multiply((0, 1, 1, own_tile), (1, 1, 1, own_tile))
    on_y(1, 1)
    on_z(1, 1)
    on_hx(2)
    on_hx(3)
    on_c(3)
    multiply((2, 1, 1, own_tile), (3, 1, 0, 0), (3, 1, 0, 1), (3, 1, 1, own_tile))
    on_y(2, 0)
    on_z(2, 0)
    on_c(4)
    multiply((4, 1, 0, 0), (4, 1, 0, 1), (4, 1, 1, own_tile))
    on_y(2, 1)
    on_z(2, 1)
    on_hend(1)
    multiply((0, 1, 1, far_tile), (1, 1, 1, far_tile), (2, 1, 1, far_tile))
    on_c(5)
    multiply((5, 1, 0, 0), (5, 1, 0, 1), (5, 1, 1, own_tile), (5, 1, 1, far_tile))
    on_y(3, 0)
    on_z(3, 1)
    on_c(6)
    multiply((6, 1, 0, 0), (6, 1, 0, 1), (6, 1, 1, own_tile), (6, 1, 1, far_tile), (3, 1, 1, far_tile), (4, 1, 1, far_tile))
    on_c(7)
    multiply((7, 1, 0, 0), (7, 1, 0, 1), (7, 1, 1, own_tile), (7, 1, 1, far_tile))

    lane = lax.broadcasted_iota(jnp.int32, (8, 128), 1)
    line = lax.broadcasted_iota(jnp.int32, (8, 128), 0)
    lse_tile = jnp.zeros((8, 128), jnp.float32)
    target_tile = jnp.zeros((8, 128), jnp.float32)
    for piece in range(2):
        peak = jnp.max(high[piece], axis=0, keepdims=True)
        summed = jnp.sum(total[piece] * jnp.exp(high[piece] - peak), axis=0, keepdims=True)
        partial = peak + jnp.log(summed)
        at_target = jnp.sum(hit_logit[piece], axis=0, keepdims=True)
        for j in range(4):
            part = slice(j * 128, (j + 1) * 128)
            here = line == piece * 4 + j
            lse_tile = jnp.where(here, jnp.broadcast_to(partial[:, part], (8, 128)), lse_tile)
            target_tile = jnp.where(here, jnp.broadcast_to(at_target[:, part], (8, 128)), target_tile)

    def swap_groups(tile):
        swapped = tile
        for d in range(1, 8):
            moved = pltpu.roll(pltpu.roll(tile, d, 0), 128 - 16 * d, 1)
            swapped = jnp.where((line - lane // 16 + 8) % 8 == d, moved, swapped)
        return swapped

    lse_tile = swap_groups(lse_tile)
    target_tile = swap_groups(target_tile)
    for r in range(8):
        msg[r, 0] = lse_tile[r:r + 1, :]
        msg[r, 1] = target_tile[r:r + 1, :]

    def to_plane(k):
        to = (vocab + k) % 8
        pltpu.make_async_remote_copy(
            src_ref=msg.at[to], dst_ref=got1.at[7 - k],
            send_sem=tail_send.at[0], recv_sem=tail_recv.at[0],
            device_id=(shadow, to), device_id_type=MESH,
        ).start()

    for k in (6, 2, 5, 7, 4, 1, 3):
        to_plane(k)
    got1[7] = msg[vocab]
    all_plane = pltpu.make_async_remote_copy(
        src_ref=msg.at[0:7], dst_ref=got1.at[0:7],
        send_sem=tail_send.at[0], recv_sem=tail_recv.at[0],
        device_id=device(0, 0, 0, 1), device_id_type=MESH,
    )
    lane = lax.broadcasted_iota(jnp.int32, (1, 128), 1)
    group = (lane % 64) // 16
    outside = jnp.zeros((1, 128), jnp.float32)
    for j in range(4):
        free = (1 - member_ref[j, vocab // 2]).astype(jnp.float32)
        outside = jnp.where(group == j, free, outside)
    msg2[2] = outside
    all_plane.wait_recv()

    pieces = got1[:, 0]
    top = jnp.max(pieces, axis=0)
    msg2[0] = top + jnp.log(jnp.sum(jnp.exp(pieces - top[None]), axis=0))
    msg2[1] = jnp.sum(got1[:, 1], axis=0)

    def to_shadows(k):
        dz, dy, dcore = k // 4, (k // 2) % 2, k % 2
        to = (((z + dz) % NZ) * 2 + (y_lo + dy) % 2) * 2 + (core + dcore) % 2
        pltpu.make_async_remote_copy(
            src_ref=msg2, dst_ref=got2.at[((NZ - dz) % NZ) * 4 + k % 4],
            send_sem=tail_send.at[1], recv_sem=tail_recv.at[1],
            device_id=(to, vocab), device_id_type=MESH,
        ).start()

    for dz in (4, 3, 5, 2, 6, 1, 7, 0):
        for k in range(max(4 * dz, 1), 4 * dz + 4):
            to_shadows(k)
    got2[0] = msg2[...]
    all_shadows = pltpu.make_async_remote_copy(
        src_ref=got2.at[1:32], dst_ref=got2.at[1:32],
        send_sem=tail_send.at[1], recv_sem=tail_recv.at[1],
        device_id=device(0, 0, 0, 1), device_id_type=MESH,
    )
    all_shadows.wait_recv()

    def both_planes(row):
        there = jnp.concatenate([got2[16:32, row], got2[0:16, row]], axis=0)
        return got2[:, row], pltpu.roll(there, 64, 2)

    here, there = both_planes(0)
    top = jnp.maximum(here, there)
    lse = top + jnp.log(jnp.exp(here - top) + jnp.exp(there - top))
    here, there = both_planes(1)
    conf = (here + there) - lse
    weighted = jnp.where(lane < 64, got2[:, 2] * conf, 0.0)
    squared = weighted * conf

    def over_groups(value):
        value = jnp.sum(value, axis=0)
        value = value + pltpu.roll(value, 64, 1)
        value = value + pltpu.roll(value, 16, 1)
        return value + pltpu.roll(value, 32, 1)

    first = over_groups(weighted)
    second = over_groups(squared)
    count = 64.0 - outside
    mean = (first - weighted[0]) / count
    variance = (second - squared[0]) / count - mean * mean
    score = (conf[0] - mean) * lax.rsqrt(jnp.maximum(variance, 0.0) + VAR_FLOOR)
    rows = jnp.broadcast_to(score, (8, 128))
    placed = rows
    for j in range(1, 4):
        placed = jnp.where(line == j, pltpu.roll(rows, 128 - 16 * j, 1), placed)
    out_ref[...] = placed[0:4, 0:16]

    for side in range(2):
        for k in range(4):
            for n in VIA_Z if k == 3 else range(CUTS):
                z_copy(k, side == 0, n).wait_send()
        for m in range(4):
            for n in range(CUTS):
                if m < 3 or n not in VIA_Z:
                    y_copy(m, side == 0, n).wait_send()
        for g in range(8):
            for n in range(CUTS):
                c_copy(g, side, n).wait_send()
    for i in range(PARTS):
        hz_copy(i).wait_send()
        hy_copy(i).wait_send()
        for part in range(2):
            for dx in (1, 3, 2):
                hx_copy(part, i, dx).wait_send()
    all_plane.wait_send()
    all_shadows.wait_send()


def per_device(hidden, targets, membership, unembedding):
    shadow_count, token_count, width = hidden.shape
    dma = pltpu.SemaphoreType.DMA
    return pl.pallas_call(
        kernel,
        out_shape=jax.ShapeDtypeStruct((4, 16), jnp.float32),
        in_specs=[pl.BlockSpec(memory_space=pltpu.HBM)] * 4,
        out_specs=pl.BlockSpec(memory_space=pltpu.VMEM),
        scratch_shapes=[
            pltpu.VMEM((1, 128), jnp.int32),
            pltpu.SMEM((4, 4), jnp.int32),
            pltpu.SMEM((32,), jnp.int32),
            pltpu.VMEM((2, 512, width), jnp.bfloat16),
            pltpu.VMEM((32, HALF, width), jnp.bfloat16),
            pltpu.VMEM((4, 8 * HALF, NT), jnp.float32),
            pltpu.VMEM((2, 8, 512), jnp.float32),
            pltpu.VMEM((2, 8, 512), jnp.float32),
            pltpu.VMEM((2, 8, 512), jnp.float32),
            pltpu.VMEM((8, NT), jnp.int32),
            pltpu.VMEM((8, 2, 1, 128), jnp.float32),
            pltpu.VMEM((8, 2, 1, 128), jnp.float32),
            pltpu.VMEM((3, 1, 128), jnp.float32),
            pltpu.VMEM((32, 3, 1, 128), jnp.float32),
            dma((4,)), dma((2, 4, CUTS)), dma((2, 4, CUTS)), dma((2, 4, CUTS)), dma((2, 4, CUTS)),
            dma((2, 8, CUTS)), dma((2, 8, CUTS)),
            dma((PARTS,)), dma((PARTS,)), dma((PARTS,)), dma((PARTS,)),
            dma((2, PARTS, 3)), dma((2, PARTS, 3)), dma((2,)), dma((2,)),
        ],
        compiler_params=pltpu.CompilerParams(
            collective_id=0, has_side_effects=True, vmem_limit_bytes=67043328
        ),
        name="score_kernel",
    )(
        hidden.reshape(shadow_count * token_count, width),
        unembedding.reshape(2, HALF, width),
        targets.reshape(1, token_count), membership,
    )


def solution(mesh):
    return jax.shard_map(
        per_device,
        mesh=mesh,
        in_specs=(P("shadow", None, None), P(), P("shadow", None), P(("shadow", "vocab"), None)),
        out_specs=P("shadow", "vocab"),
        check_vma=False,
    )
```

```python
import functools

import jax
import jax.numpy as jnp
from jax import lax
from jax.experimental import pallas as pl
from jax.experimental.pallas import tpu as pltpu
from jax.sharding import PartitionSpec as P

NEG_FILL = -1e30
VAR_FLOOR = 0.5
MESH = pl.DeviceIdType.MESH
NZ = 8
HALF = 64
NT = 256
PARTS = 4
ROWS = 64 // PARTS
CUTS = 2
CUT = HALF // CUTS
VIA_Z = (1,)
FIRST_X = (1, 3, 2)

GROUPS = (
    ((0, 0, 0), (0, 0, 1)),
    ((0, -1, 0), (0, 1, 1)),
    ((-1, 0, 0), (1, 0, 1)),
    ((-1, -1, 0), (1, 1, 1)),
    ((-1, 0, 1), (1, 0, 0)),
    ((1, -1, 0), (-1, 1, 1)),
    ((-2, 0, 0), (2, 0, 1)),
    ((-2, -1, 0), (2, 1, 1)),
)


def kernel(
    hidden_hbm, head_hbm, targets_hbm, member_hbm, out_ref,
    targets_ref, member_ref, bases, hid, head, logits, high, total, hit_logit, tg,
    msg, got1, msg2, got2,
    local_sem, z_send, z_recv, y_send, y_recv, c_send, c_recv,
    hz_send, hz_recv, hy_send, hy_recv, hx_send, hx_recv, tail_send, tail_recv,
):
    shadow = lax.axis_index("shadow")
    vocab = lax.axis_index("vocab")
    z = shadow // 4
    y_lo = (shadow // 2) % 2
    core = shadow % 2
    y_hi = vocab // 4
    x = vocab % 4
    y = y_hi * 2 + y_lo

    def device(dz, dy, dx, dcore):
        to_y = (y + dy) % 4
        return (
            (((z + dz) % NZ) * 2 + to_y % 2) * 2 + (core + dcore) % 2,
            (to_y // 2) * 4 + (x + dx) % 4,
        )

    own_head = pltpu.make_async_copy(head_hbm, head.at[pl.ds(0, 2)], local_sem.at[0])
    own_hid = pltpu.make_async_copy(hidden_hbm, hid.at[0], local_sem.at[1])
    own_tg = pltpu.make_async_copy(targets_hbm, targets_ref, local_sem.at[2])
    own_member = pltpu.make_async_copy(member_hbm, member_ref, local_sem.at[3])
    own_head.start()
    own_hid.start()
    own_tg.start()
    own_member.start()

    barrier = pltpu.get_barrier_semaphore()
    near = ((1, 0, 0, 0), (7, 0, 0, 0), (4, 0, 0, 0), (0, 1, 0, 0), (0, 3, 0, 0), (0, 2, 0, 0), (0, 0, 1, 0), (0, 0, 3, 0), (0, 0, 2, 0), (0, 0, 0, 1))
    for offset in near:
        pl.semaphore_signal(barrier, inc=1, device_id=device(*offset), device_id_type=MESH)

    high[...] = jnp.full_like(high, NEG_FILL)
    total[...] = jnp.zeros_like(total)
    hit_logit[...] = jnp.zeros_like(hit_logit)
    for g in range(8):
        for u in range(4):
            dz, dy, half = GROUPS[g][u % 2]
            at_y = (y + dy + 4) % 4
            block = ((((z + dz + NZ) % NZ) * 2 + at_y % 2) * 2 + (core + u // 2) % 2) * 8 + (at_y // 2) * 4 + x
            bases[4 * g + u] = block * (2 * HALF) + half * HALF
    own_tg.wait()
    own_member.wait()
    wide = jnp.broadcast_to(targets_ref[...], (8, 128))
    tg[:, 0:128] = wide
    tg[:, 128:256] = wide

    def z_copy(k, upward, n):
        rows = pl.ds(n * CUT, CUT)
        side = 0 if upward else 1
        src = (side, 1 - side, 8 + side, 12 + side)[k]
        dst = (8, 16, 24, 28)[k] + side
        return pltpu.make_async_remote_copy(
            src_ref=head.at[src, rows, :], dst_ref=head.at[dst, rows, :],
            send_sem=z_send.at[side, k, n], recv_sem=z_recv.at[side, k, n],
            device_id=device(1 if upward else NZ - 1, 0, 0, 0), device_id_type=MESH,
        )

    def y_copy(m, upward, n):
        rows = pl.ds(n * CUT, CUT)
        side = 0 if upward else 1
        src = ((0, 8, 17, 24) if upward else (1, 9, 16, 25))[m]
        return pltpu.make_async_remote_copy(
            src_ref=head.at[src, rows, :], dst_ref=head.at[8 * m + 4 + side, rows, :],
            send_sem=y_send.at[side, m, n], recv_sem=y_recv.at[side, m, n],
            device_id=device(0, 1 if upward else 3, 0, 0), device_id_type=MESH,
        )

    def c_copy(g, side, n):
        rows = pl.ds(n * CUT, CUT)
        return pltpu.make_async_remote_copy(
            src_ref=head.at[4 * g + side, rows, :], dst_ref=head.at[4 * g + 2 + side, rows, :],
            send_sem=c_send.at[side, g, n], recv_sem=c_recv.at[side, g, n],
            device_id=device(0, 0, 0, 1), device_id_type=MESH,
        )

    def hz_copy(i):
        rows = pl.ds(pl.multiple_of(vocab * 64 + i * ROWS, ROWS), ROWS)
        return pltpu.make_async_remote_copy(
            src_ref=hid.at[0, rows, :], dst_ref=hid.at[1, rows, :],
            send_sem=hz_send.at[i], recv_sem=hz_recv.at[i],
            device_id=device(4, 0, 0, 0), device_id_type=MESH,
        )

    def hy_copy(i):
        rows = pl.ds(pl.multiple_of(vocab * 64 + i * ROWS, ROWS), ROWS)
        return pltpu.make_async_remote_copy(
            src_ref=hid.at[1, rows, :], dst_ref=hid.at[1, rows, :],
            send_sem=hy_send.at[i], recv_sem=hy_recv.at[i],
            device_id=device(0, 2, 0, 0), device_id_type=MESH,
        )

    def hx_copy(part, i, dx):
        to_x, owner = dx, x
        if part == 1 and dx == 2:
            to_x = 1 if i % 2 == 0 else 3
            owner = (x + 4 - to_x) % 4
        share = ((y_hi + part) % 2) * 4 + owner
        rows = pl.ds(pl.multiple_of(share * 64 + i * ROWS, ROWS), ROWS)
        return pltpu.make_async_remote_copy(
            src_ref=hid.at[1, rows, :], dst_ref=hid.at[1, rows, :],
            send_sem=hx_send.at[part, i, dx - 1], recv_sem=hx_recv.at[part, i, dx - 1],
            device_id=device(0, 0, to_x, 0), device_id_type=MESH,
        )

    def columns(tile):
        return pl.ds(pl.multiple_of(tile * NT, NT), NT)

    def product(g, count, piece, tile, buf):
        lhs = head[4 * g:4 * (g + count)].reshape(4 * count * HALF, head.shape[2])
        rhs = hid[piece, columns(tile), :]
        logits[buf, 0:4 * count * HALF] = lax.dot_general(
            lhs, rhs, (((1,), (1,)), ((), ())), preferred_element_type=jnp.float32
        )

    def fold(first, count, piece, tile, buf):
        for g in range(first, first + count):
            fold_group(g, (g - first) * 4, piece, columns(tile), buf)

    def fold_group(g, at, piece, cols, buf):
        ids = lax.broadcasted_iota(jnp.int32, (8, 8, NT), 1) + 8 * lax.broadcasted_iota(
            jnp.int32, (8, 8, NT), 0
        )
        found = hit_logit[piece, :, cols]
        others = []
        old = high[piece, :, cols]
        new = old
        for u in range(4):
            v = logits[buf, (at + u) * HALF:(at + u + 1) * HALF, :].reshape(8, 8, NT)
            hit = (tg[...] - bases[4 * g + u])[None] == ids
            found = found + jnp.sum(jnp.where(hit, v, 0.0), axis=0)
            v = jnp.where(hit, 2.0 * NEG_FILL, v)
            new = jnp.maximum(new, jnp.max(v, axis=0))
            others.append(v)
        fresh = total[piece, :, cols] * jnp.exp(old - new)
        for v in others:
            fresh = fresh + jnp.sum(jnp.exp(v - new[None]), axis=0)
        high[piece, :, cols] = new
        total[piece, :, cols] = fresh
        hit_logit[piece, :, cols] = found

    def multiply(*tiles):
        for i, tile in enumerate(tiles):
            product(*tile, i % 4)
            if i:
                fold(*tiles[i - 1], (i - 1) % 4)
        fold(*tiles[-1], (len(tiles) - 1) % 4)

    own_tile, far_tile = y_hi, 1 - y_hi

    def on_z(k, n):
        for side in range(2):
            upward = side == 0
            z_copy(k, upward, n).wait_recv()
            if k == 0:
                z_copy(2, upward, n).start()
            if k < 2 or (k == 2 and n not in VIA_Z):
                y_copy(k + 1, upward == (k != 1), n).start()
            c_copy(7 if k == 3 else 2 * k + 2, side, n).start()

    def on_y(m, n):
        for side in range(2):
            y_copy(m, side == 0, n).wait_recv()
            if m == 1 and n in VIA_Z:
                z_copy(3, side == 0, n).start()
            c_copy(2 * m + 1, side, n).start()

    def on_c(g):
        for side in range(2):
            for n in range(CUTS):
                c_copy(g, side, n).wait_recv()

    def on_hz(i):
        hz_copy(i).wait_recv()
        hy_copy(i).start()
        for dx in FIRST_X:
            hx_copy(0, i, dx).start()

    def on_hy(i):
        hy_copy(i).wait_recv()
        for dx in (1, 3):
            hx_copy(1, i, dx).start()

    def on_hx(i):
        for dx in (1, 3):
            hx_copy(1, i, dx).wait_recv()
            if (dx == 1) == (i % 2 == 0):
                hx_copy(1, i, 2).start()

    def on_hend(part):
        for i in range(PARTS):
            for dx in (1, 3, 2) if part == 0 else (2,):
                hx_copy(part, i, dx).wait_recv()

    pl.semaphore_wait(barrier, len(near))
    own_head.wait()
    for n in range(CUTS):
        c_copy(0, 0, n).start()
        c_copy(0, 1, n).start()
    for n in range(CUTS):
        y_copy(0, True, n).start()
        y_copy(0, False, n).start()
    own_hid.wait()
    hz_copy(0).start()
    hz_copy(1).start()
    hz_copy(2).start()
    hz_copy(3).start()
    z_copy(0, True, 0).start()
    z_copy(0, False, 0).start()
    z_copy(0, True, 1).start()
    z_copy(0, False, 1).start()
    z_copy(1, True, 0).start()
    z_copy(1, False, 0).start()
    z_copy(1, True, 1).start()
    z_copy(1, False, 1).start()
    on_c(0)
    multiply((0, 1, 0, 0), (0, 1, 0, 1))
    on_y(0, 0)
    on_hz(0)
    on_y(0, 1)
    on_c(1)
    multiply((1, 1, 0, 0), (1, 1, 0, 1))
    on_hz(1)
    on_hz(2)
    on_hz(3)
    on_hy(0)
    on_hy(1)
    on_z(0, 0)
    on_hy(2)
    on_z(0, 1)
    on_hy(3)
    on_c(2)
    multiply((2, 1, 0, 0), (2, 1, 0, 1))
    on_y(1, 0)
    on_z(1, 0)
    on_hx(0)
    on_hx(1)
    on_hend(0)
    multiply((0, 1, 1, own_tile), (1, 1, 1, own_tile))
    on_y(1, 1)
    on_z(1, 1)
    on_hx(2)
    on_hx(3)
    on_c(3)
    multiply((2, 1, 1, own_tile), (3, 1, 0, 0), (3, 1, 0, 1), (3, 1, 1, own_tile))
    on_y(2, 0)
    on_z(2, 0)
    on_c(4)
    multiply((4, 1, 0, 0), (4, 1, 0, 1), (4, 1, 1, own_tile))
    on_y(2, 1)
    on_z(2, 1)
    on_hend(1)
    multiply((0, 1, 1, far_tile), (1, 1, 1, far_tile), (2, 1, 1, far_tile))
    on_c(5)
    multiply((5, 1, 0, 0), (5, 1, 0, 1), (5, 1, 1, own_tile), (5, 1, 1, far_tile))
    on_y(3, 0)
    on_z(3, 1)
    on_c(6)
    multiply((6, 1, 0, 0), (6, 1, 0, 1), (6, 1, 1, own_tile), (6, 1, 1, far_tile), (3, 1, 1, far_tile), (4, 1, 1, far_tile))
    on_c(7)
    multiply((7, 1, 0, 0), (7, 1, 0, 1), (7, 1, 1, own_tile), (7, 1, 1, far_tile))

    lane = lax.broadcasted_iota(jnp.int32, (8, 128), 1)
    line = lax.broadcasted_iota(jnp.int32, (8, 128), 0)
    lse_tile = jnp.zeros((8, 128), jnp.float32)
    target_tile = jnp.zeros((8, 128), jnp.float32)
    for piece in range(2):
        peak = jnp.max(high[piece], axis=0, keepdims=True)
        summed = jnp.sum(total[piece] * jnp.exp(high[piece] - peak), axis=0, keepdims=True)
        partial = peak + jnp.log(summed)
        at_target = jnp.sum(hit_logit[piece], axis=0, keepdims=True)
        for j in range(4):
            part = slice(j * 128, (j + 1) * 128)
            here = line == piece * 4 + j
            lse_tile = jnp.where(here, jnp.broadcast_to(partial[:, part], (8, 128)), lse_tile)
            target_tile = jnp.where(here, jnp.broadcast_to(at_target[:, part], (8, 128)), target_tile)

    def swap_groups(tile):
        swapped = tile
        for d in range(1, 8):
            moved = pltpu.roll(pltpu.roll(tile, d, 0), 128 - 16 * d, 1)
            swapped = jnp.where((line - lane // 16 + 8) % 8 == d, moved, swapped)
        return swapped

    lse_tile = swap_groups(lse_tile)
    target_tile = swap_groups(target_tile)
    for r in range(8):
        msg[r, 0] = lse_tile[r:r + 1, :]
        msg[r, 1] = target_tile[r:r + 1, :]

    def to_plane(k):
        to = (vocab + k) % 8
        pltpu.make_async_remote_copy(
            src_ref=msg.at[to], dst_ref=got1.at[7 - k],
            send_sem=tail_send.at[0], recv_sem=tail_recv.at[0],
            device_id=(shadow, to), device_id_type=MESH,
        ).start()

    for k in (6, 2, 5, 7, 4, 1, 3):
        to_plane(k)
    got1[7] = msg[vocab]
    all_plane = pltpu.make_async_remote_copy(
        src_ref=msg.at[0:7], dst_ref=got1.at[0:7],
        send_sem=tail_send.at[0], recv_sem=tail_recv.at[0],
        device_id=device(0, 0, 0, 1), device_id_type=MESH,
    )
    lane = lax.broadcasted_iota(jnp.int32, (1, 128), 1)
    group = (lane % 64) // 16
    outside = jnp.zeros((1, 128), jnp.float32)
    for j in range(4):
        free = (1 - member_ref[j, vocab // 2]).astype(jnp.float32)
        outside = jnp.where(group == j, free, outside)
    msg2[2] = outside
    all_plane.wait_recv()

    pieces = got1[:, 0]
    top = jnp.max(pieces, axis=0)
    msg2[0] = top + jnp.log(jnp.sum(jnp.exp(pieces - top[None]), axis=0))
    msg2[1] = jnp.sum(got1[:, 1], axis=0)

    def to_shadows(k):
        dz, dy, dcore = k // 4, (k // 2) % 2, k % 2
        to = (((z + dz) % NZ) * 2 + (y_lo + dy) % 2) * 2 + (core + dcore) % 2
        pltpu.make_async_remote_copy(
            src_ref=msg2, dst_ref=got2.at[((NZ - dz) % NZ) * 4 + k % 4],
            send_sem=tail_send.at[1], recv_sem=tail_recv.at[1],
            device_id=(to, vocab), device_id_type=MESH,
        ).start()

    for dz in (4, 3, 5, 2, 6, 1, 7, 0):
        for k in range(max(4 * dz, 1), 4 * dz + 4):
            to_shadows(k)
    got2[0] = msg2[...]
    all_shadows = pltpu.make_async_remote_copy(
        src_ref=got2.at[1:32], dst_ref=got2.at[1:32],
        send_sem=tail_send.at[1], recv_sem=tail_recv.at[1],
        device_id=device(0, 0, 0, 1), device_id_type=MESH,
    )
    all_shadows.wait_recv()

    def both_planes(row):
        there = jnp.concatenate([got2[16:32, row], got2[0:16, row]], axis=0)
        return got2[:, row], pltpu.roll(there, 64, 2)

    here, there = both_planes(0)
    top = jnp.maximum(here, there)
    lse = top + jnp.log(jnp.exp(here - top) + jnp.exp(there - top))
    here, there = both_planes(1)
    conf = (here + there) - lse
    weighted = jnp.where(lane < 64, got2[:, 2] * conf, 0.0)
    squared = weighted * conf

    def over_groups(value):
        value = jnp.sum(value, axis=0)
        value = value + pltpu.roll(value, 64, 1)
        value = value + pltpu.roll(value, 16, 1)
        return value + pltpu.roll(value, 32, 1)

    first = over_groups(weighted)
    second = over_groups(squared)
    count = 64.0 - outside
    mean = (first - weighted[0]) / count
    variance = (second - squared[0]) / count - mean * mean
    score = (conf[0] - mean) * lax.rsqrt(jnp.maximum(variance, 0.0) + VAR_FLOOR)
    rows = jnp.broadcast_to(score, (8, 128))
    placed = rows
    for j in range(1, 4):
        placed = jnp.where(line == j, pltpu.roll(rows, 128 - 16 * j, 1), placed)
    out_ref[...] = placed[0:4, 0:16]

    for side in range(2):
        for k in range(4):
            for n in VIA_Z if k == 3 else range(CUTS):
                z_copy(k, side == 0, n).wait_send()
        for m in range(4):
            for n in range(CUTS):
                if m < 3 or n not in VIA_Z:
                    y_copy(m, side == 0, n).wait_send()
        for g in range(8):
            for n in range(CUTS):
                c_copy(g, side, n).wait_send()
    for i in range(PARTS):
        hz_copy(i).wait_send()
        hy_copy(i).wait_send()
        for part in range(2):
            for dx in (1, 3, 2):
                hx_copy(part, i, dx).wait_send()
    all_plane.wait_send()
    all_shadows.wait_send()


def per_device(hidden, targets, membership, unembedding):
    shadow_count, token_count, width = hidden.shape
    dma = pltpu.SemaphoreType.DMA
    return pl.pallas_call(
        kernel,
        out_shape=pltpu.VMEM((4, 16), jnp.float32),
        in_specs=[pl.BlockSpec(memory_space=pltpu.HBM)] * 4,
        out_specs=pl.BlockSpec(memory_space=pltpu.VMEM),
        scratch_shapes=[
            pltpu.VMEM((1, 128), jnp.int32),
            pltpu.SMEM((4, 4), jnp.int32),
            pltpu.SMEM((32,), jnp.int32),
            pltpu.VMEM((2, 512, width), jnp.bfloat16),
            pltpu.VMEM((32, HALF, width), jnp.bfloat16),
            pltpu.VMEM((4, 8 * HALF, NT), jnp.float32),
            pltpu.VMEM((2, 8, 512), jnp.float32),
            pltpu.VMEM((2, 8, 512), jnp.float32),
            pltpu.VMEM((2, 8, 512), jnp.float32),
            pltpu.VMEM((8, NT), jnp.int32),
            pltpu.VMEM((8, 2, 1, 128), jnp.float32),
            pltpu.VMEM((8, 2, 1, 128), jnp.float32),
            pltpu.VMEM((3, 1, 128), jnp.float32),
            pltpu.VMEM((32, 3, 1, 128), jnp.float32),
            dma((4,)), dma((2, 4, CUTS)), dma((2, 4, CUTS)), dma((2, 4, CUTS)), dma((2, 4, CUTS)),
            dma((2, 8, CUTS)), dma((2, 8, CUTS)),
            dma((PARTS,)), dma((PARTS,)), dma((PARTS,)), dma((PARTS,)),
            dma((2, PARTS, 3)), dma((2, PARTS, 3)), dma((2,)), dma((2,)),
        ],
        compiler_params=pltpu.CompilerParams(
            collective_id=0, has_side_effects=True, vmem_limit_bytes=60 * 2**20
        ),
        name="score_kernel",
    )(*(pltpu.with_memory_space_constraint(a, pltpu.HBM) for a in (
        hidden.reshape(shadow_count * token_count, width),
        unembedding.reshape(2, HALF, width),
        targets.reshape(1, token_count), membership,
    )))


def solution(mesh):
    return jax.shard_map(
        per_device,
        mesh=mesh,
        in_specs=(P("shadow", None, None), P(), P("shadow", None), P(("shadow", "vocab"), None)),
        out_specs=P("shadow", "vocab"),
        check_vma=False,
    )
```

```python
import functools

import jax
import jax.numpy as jnp
from jax import lax
from jax.experimental import pallas as pl
from jax.experimental.pallas import tpu as pltpu
from jax.sharding import PartitionSpec as P

NEG_FILL = -1e30
VAR_FLOOR = 0.5
MESH = pl.DeviceIdType.MESH
NZ = 8
HALF = 64
NT = 256
PARTS = 4
ROWS = 64 // PARTS
CUTS = 2
CUT = HALF // CUTS
VIA_Z = (1,)
FIRST_X = (1, 3, 2)

GROUPS = (
    ((0, 0, 0), (0, 0, 1)),
    ((0, -1, 0), (0, 1, 1)),
    ((-1, 0, 0), (1, 0, 1)),
    ((-1, -1, 0), (1, 1, 1)),
    ((-1, 0, 1), (1, 0, 0)),
    ((1, -1, 0), (-1, 1, 1)),
    ((-2, 0, 0), (2, 0, 1)),
    ((-2, -1, 0), (2, 1, 1)),
)


def kernel(
    hidden_hbm, head_hbm, targets_hbm, member_hbm, out_ref,
    targets_ref, member_ref, bases, hid, head, logits, high, total, hit_logit, tg,
    msg, got1, msg2, got2,
    local_sem, z_send, z_recv, y_send, y_recv, c_send, c_recv,
    hz_send, hz_recv, hy_send, hy_recv, hx_send, hx_recv, tail_send, tail_recv,
):
    shadow = lax.axis_index("shadow")
    vocab = lax.axis_index("vocab")
    z = shadow // 4
    y_lo = (shadow // 2) % 2
    core = shadow % 2
    y_hi = vocab // 4
    x = vocab % 4
    y = y_hi * 2 + y_lo

    def device(dz, dy, dx, dcore):
        to_y = (y + dy) % 4
        return (
            (((z + dz) % NZ) * 2 + to_y % 2) * 2 + (core + dcore) % 2,
            (to_y // 2) * 4 + (x + dx) % 4,
        )

    barrier = pltpu.get_barrier_semaphore()
    near = ((4, 0, 0, 0), (1, 0, 0, 0), (7, 0, 0, 0), (0, 1, 0, 0), (0, 3, 0, 0), (0, 2, 0, 0), (0, 0, 1, 0), (0, 0, 3, 0), (0, 0, 2, 0), (0, 0, 0, 1))
    for offset in near:
        pl.semaphore_signal(barrier, inc=1, device_id=device(*offset), device_id_type=MESH)

    own_head = pltpu.make_async_copy(head_hbm, head.at[pl.ds(0, 2)], local_sem.at[0])
    own_hid = pltpu.make_async_copy(hidden_hbm, hid.at[0], local_sem.at[1])
    own_tg = pltpu.make_async_copy(targets_hbm, targets_ref, local_sem.at[2])
    own_member = pltpu.make_async_copy(member_hbm, member_ref, local_sem.at[3])
    own_head.start()
    own_hid.start()
    own_tg.start()
    own_member.start()

    high[...] = jnp.full_like(high, NEG_FILL)
    total[...] = jnp.zeros_like(total)
    hit_logit[...] = jnp.zeros_like(hit_logit)
    for g in range(8):
        for u in range(4):
            dz, dy, half = GROUPS[g][u % 2]
            at_y = (y + dy + 4) % 4
            block = ((((z + dz + NZ) % NZ) * 2 + at_y % 2) * 2 + (core + u // 2) % 2) * 8 + (at_y // 2) * 4 + x
            bases[4 * g + u] = block * (2 * HALF) + half * HALF
    own_tg.wait()
    own_member.wait()
    wide = jnp.broadcast_to(targets_ref[...], (8, 128))
    tg[:, 0:128] = wide
    tg[:, 128:256] = wide

    def z_copy(k, upward, n):
        rows = pl.ds(n * CUT, CUT)
        side = 0 if upward else 1
        src = (side, 1 - side, 8 + side, 12 + side)[k]
        dst = (8, 16, 24, 28)[k] + side
        return pltpu.make_async_remote_copy(
            src_ref=head.at[src, rows, :], dst_ref=head.at[dst, rows, :],
            send_sem=z_send.at[side, k, n], recv_sem=z_recv.at[side, k, n],
            device_id=device(1 if upward else NZ - 1, 0, 0, 0), device_id_type=MESH,
        )

    def y_copy(m, upward, n):
        rows = pl.ds(n * CUT, CUT)
        side = 0 if upward else 1
        src = ((0, 8, 17, 24) if upward else (1, 9, 16, 25))[m]
        return pltpu.make_async_remote_copy(
            src_ref=head.at[src, rows, :], dst_ref=head.at[8 * m + 4 + side, rows, :],
            send_sem=y_send.at[side, m, n], recv_sem=y_recv.at[side, m, n],
            device_id=device(0, 1 if upward else 3, 0, 0), device_id_type=MESH,
        )

    def c_copy(g, side, n):
        rows = pl.ds(n * CUT, CUT)
        return pltpu.make_async_remote_copy(
            src_ref=head.at[4 * g + side, rows, :], dst_ref=head.at[4 * g + 2 + side, rows, :],
            send_sem=c_send.at[side, g, n], recv_sem=c_recv.at[side, g, n],
            device_id=device(0, 0, 0, 1), device_id_type=MESH,
        )

    def hz_copy(i):
        rows = pl.ds(pl.multiple_of(vocab * 64 + i * ROWS, ROWS), ROWS)
        return pltpu.make_async_remote_copy(
            src_ref=hid.at[0, rows, :], dst_ref=hid.at[1, rows, :],
            send_sem=hz_send.at[i], recv_sem=hz_recv.at[i],
            device_id=device(4, 0, 0, 0), device_id_type=MESH,
        )

    def hy_copy(i):
        rows = pl.ds(pl.multiple_of(vocab * 64 + i * ROWS, ROWS), ROWS)
        return pltpu.make_async_remote_copy(
            src_ref=hid.at[1, rows, :], dst_ref=hid.at[1, rows, :],
            send_sem=hy_send.at[i], recv_sem=hy_recv.at[i],
            device_id=device(0, 2, 0, 0), device_id_type=MESH,
        )

    def hx_copy(part, i, dx):
        to_x, owner = dx, x
        if part == 1 and dx == 2:
            to_x = 1 if i % 2 == 0 else 3
            owner = (x + 4 - to_x) % 4
        share = ((y_hi + part) % 2) * 4 + owner
        rows = pl.ds(pl.multiple_of(share * 64 + i * ROWS, ROWS), ROWS)
        return pltpu.make_async_remote_copy(
            src_ref=hid.at[1, rows, :], dst_ref=hid.at[1, rows, :],
            send_sem=hx_send.at[part, i, dx - 1], recv_sem=hx_recv.at[part, i, dx - 1],
            device_id=device(0, 0, to_x, 0), device_id_type=MESH,
        )

    def columns(tile):
        return pl.ds(pl.multiple_of(tile * NT, NT), NT)

    def product(g, count, piece, tile, buf):
        lhs = head[4 * g:4 * (g + count)].reshape(4 * count * HALF, head.shape[2])
        rhs = hid[piece, columns(tile), :]
        logits[buf, 0:4 * count * HALF] = lax.dot_general(
            lhs, rhs, (((1,), (1,)), ((), ())), preferred_element_type=jnp.float32
        )

    def fold(first, count, piece, tile, buf):
        for g in range(first, first + count):
            fold_group(g, (g - first) * 4, piece, columns(tile), buf)

    def fold_group(g, at, piece, cols, buf):
        ids = lax.broadcasted_iota(jnp.int32, (8, 8, NT), 1) + 8 * lax.broadcasted_iota(
            jnp.int32, (8, 8, NT), 0
        )
        found = hit_logit[piece, :, cols]
        others = []
        old = high[piece, :, cols]
        new = old
        for u in range(4):
            v = logits[buf, (at + u) * HALF:(at + u + 1) * HALF, :].reshape(8, 8, NT)
            hit = (tg[...] - bases[4 * g + u])[None] == ids
            found = found + jnp.sum(jnp.where(hit, v, 0.0), axis=0)
            v = jnp.where(hit, 2.0 * NEG_FILL, v)
            new = jnp.maximum(new, jnp.max(v, axis=0))
            others.append(v)
        fresh = total[piece, :, cols] * jnp.exp(old - new)
        for v in others:
            fresh = fresh + jnp.sum(jnp.exp(v - new[None]), axis=0)
        high[piece, :, cols] = new
        total[piece, :, cols] = fresh
        hit_logit[piece, :, cols] = found

    def multiply(*tiles):
        for i, tile in enumerate(tiles):
            product(*tile, i % 4)
            if i:
                fold(*tiles[i - 1], (i - 1) % 4)
        fold(*tiles[-1], (len(tiles) - 1) % 4)

    own_tile, far_tile = y_hi, 1 - y_hi

    def on_z(k, n):
        for side in range(2):
            upward = side == 0
            z_copy(k, upward, n).wait_recv()
            if k == 0:
                z_copy(2, upward, n).start()
            if k < 2 or (k == 2 and n not in VIA_Z):
                y_copy(k + 1, upward == (k != 1), n).start()
            c_copy(7 if k == 3 else 2 * k + 2, side, n).start()

    def on_y(m, n):
        for side in range(2):
            y_copy(m, side == 0, n).wait_recv()
            if m == 1 and n in VIA_Z:
                z_copy(3, side == 0, n).start()
            c_copy(2 * m + 1, side, n).start()

    def on_c(g):
        for side in range(2):
            for n in range(CUTS):
                c_copy(g, side, n).wait_recv()

    def on_hz(i):
        hz_copy(i).wait_recv()
        hy_copy(i).start()
        for dx in FIRST_X:
            hx_copy(0, i, dx).start()

    def on_hy(i):
        hy_copy(i).wait_recv()
        for dx in (1, 3):
            hx_copy(1, i, dx).start()

    def on_hx(i):
        for dx in (1, 3):
            hx_copy(1, i, dx).wait_recv()
            if (dx == 1) == (i % 2 == 0):
                hx_copy(1, i, 2).start()

    def on_hend(part):
        for i in range(PARTS):
            for dx in (1, 3, 2) if part == 0 else (2,):
                hx_copy(part, i, dx).wait_recv()

    pl.semaphore_wait(barrier, len(near))
    own_head.wait()
    own_hid.wait()
    hz_copy(0).start()
    hz_copy(1).start()
    hz_copy(2).start()
    hz_copy(3).start()
    z_copy(0, True, 0).start()
    z_copy(0, False, 0).start()
    z_copy(0, True, 1).start()
    z_copy(0, False, 1).start()
    z_copy(1, True, 0).start()
    z_copy(1, False, 0).start()
    z_copy(1, True, 1).start()
    z_copy(1, False, 1).start()
    for n in range(CUTS):
        c_copy(0, 0, n).start()
        c_copy(0, 1, n).start()
    for n in range(CUTS):
        y_copy(0, True, n).start()
        y_copy(0, False, n).start()
    on_c(0)
    multiply((0, 1, 0, 0), (0, 1, 0, 1))
    on_y(0, 0)
    on_hz(0)
    on_y(0, 1)
    on_c(1)
    multiply((1, 1, 0, 0), (1, 1, 0, 1))
    on_hz(1)
    on_hz(2)
    on_hz(3)
    on_hy(0)
    on_hy(1)
    on_z(0, 0)
    on_hy(2)
    on_z(0, 1)
    on_hy(3)
    on_c(2)
    multiply((2, 1, 0, 0), (2, 1, 0, 1))
    on_y(1, 0)
    on_z(1, 0)
    on_hx(0)
    on_hx(1)
    on_hend(0)
    multiply((0, 1, 1, own_tile), (1, 1, 1, own_tile))
    on_y(1, 1)
    on_z(1, 1)
    on_hx(2)
    on_hx(3)
    on_c(3)
    multiply((2, 1, 1, own_tile), (3, 1, 0, 0), (3, 1, 0, 1), (3, 1, 1, own_tile))
    on_y(2, 0)
    on_z(2, 0)
    on_c(4)
    multiply((4, 1, 0, 0), (4, 1, 0, 1), (4, 1, 1, own_tile))
    on_y(2, 1)
    on_z(2, 1)
    on_hend(1)
    multiply((0, 1, 1, far_tile), (1, 1, 1, far_tile), (2, 1, 1, far_tile))
    on_c(5)
    multiply((5, 1, 0, 0), (5, 1, 0, 1), (5, 1, 1, own_tile), (5, 1, 1, far_tile))
    on_y(3, 0)
    on_z(3, 1)
    on_c(6)
    multiply((6, 1, 0, 0), (6, 1, 0, 1), (6, 1, 1, own_tile), (6, 1, 1, far_tile), (3, 1, 1, far_tile), (4, 1, 1, far_tile))
    on_c(7)
    multiply((7, 1, 0, 0), (7, 1, 0, 1), (7, 1, 1, own_tile), (7, 1, 1, far_tile))

    lane = lax.broadcasted_iota(jnp.int32, (8, 128), 1)
    line = lax.broadcasted_iota(jnp.int32, (8, 128), 0)
    lse_tile = jnp.zeros((8, 128), jnp.float32)
    target_tile = jnp.zeros((8, 128), jnp.float32)
    for piece in range(2):
        peak = jnp.max(high[piece], axis=0, keepdims=True)
        summed = jnp.sum(total[piece] * jnp.exp(high[piece] - peak), axis=0, keepdims=True)
        partial = peak + jnp.log(summed)
        at_target = jnp.sum(hit_logit[piece], axis=0, keepdims=True)
        for j in range(4):
            part = slice(j * 128, (j + 1) * 128)
            here = line == piece * 4 + j
            lse_tile = jnp.where(here, jnp.broadcast_to(partial[:, part], (8, 128)), lse_tile)
            target_tile = jnp.where(here, jnp.broadcast_to(at_target[:, part], (8, 128)), target_tile)

    def swap_groups(tile):
        swapped = tile
        for d in range(1, 8):
            moved = pltpu.roll(pltpu.roll(tile, d, 0), 128 - 16 * d, 1)
            swapped = jnp.where((line - lane // 16 + 8) % 8 == d, moved, swapped)
        return swapped

    lse_tile = swap_groups(lse_tile)
    target_tile = swap_groups(target_tile)
    for r in range(8):
        msg[r, 0] = lse_tile[r:r + 1, :]
        msg[r, 1] = target_tile[r:r + 1, :]

    def to_plane(k):
        to = (vocab + k) % 8
        pltpu.make_async_remote_copy(
            src_ref=msg.at[to], dst_ref=got1.at[7 - k],
            send_sem=tail_send.at[0], recv_sem=tail_recv.at[0],
            device_id=(shadow, to), device_id_type=MESH,
        ).start()

    for k in (6, 2, 5, 7, 4, 1, 3):
        to_plane(k)
    got1[7] = msg[vocab]
    all_plane = pltpu.make_async_remote_copy(
        src_ref=msg.at[0:7], dst_ref=got1.at[0:7],
        send_sem=tail_send.at[0], recv_sem=tail_recv.at[0],
        device_id=device(0, 0, 0, 1), device_id_type=MESH,
    )
    lane = lax.broadcasted_iota(jnp.int32, (1, 128), 1)
    group = (lane % 64) // 16
    outside = jnp.zeros((1, 128), jnp.float32)
    for j in range(4):
        free = (1 - member_ref[j, vocab // 2]).astype(jnp.float32)
        outside = jnp.where(group == j, free, outside)
    msg2[2] = outside
    all_plane.wait_recv()

    pieces = got1[:, 0]
    top = jnp.max(pieces, axis=0)
    msg2[0] = top + jnp.log(jnp.sum(jnp.exp(pieces - top[None]), axis=0))
    msg2[1] = jnp.sum(got1[:, 1], axis=0)

    def to_shadows(k):
        dz, dy, dcore = k // 4, (k // 2) % 2, k % 2
        to = (((z + dz) % NZ) * 2 + (y_lo + dy) % 2) * 2 + (core + dcore) % 2
        pltpu.make_async_remote_copy(
            src_ref=msg2, dst_ref=got2.at[((NZ - dz) % NZ) * 4 + k % 4],
            send_sem=tail_send.at[1], recv_sem=tail_recv.at[1],
            device_id=(to, vocab), device_id_type=MESH,
        ).start()

    for dz in (4, 3, 5, 2, 6, 1, 7, 0):
        for k in range(max(4 * dz, 1), 4 * dz + 4):
            to_shadows(k)
    got2[0] = msg2[...]
    all_shadows = pltpu.make_async_remote_copy(
        src_ref=got2.at[1:32], dst_ref=got2.at[1:32],
        send_sem=tail_send.at[1], recv_sem=tail_recv.at[1],
        device_id=device(0, 0, 0, 1), device_id_type=MESH,
    )
    all_shadows.wait_recv()

    def both_planes(row):
        there = jnp.concatenate([got2[16:32, row], got2[0:16, row]], axis=0)
        return got2[:, row], pltpu.roll(there, 64, 2)

    here, there = both_planes(0)
    top = jnp.maximum(here, there)
    lse = top + jnp.log(jnp.exp(here - top) + jnp.exp(there - top))
    here, there = both_planes(1)
    conf = (here + there) - lse
    weighted = jnp.where(lane < 64, got2[:, 2] * conf, 0.0)
    squared = weighted * conf

    def over_groups(value):
        value = jnp.sum(value, axis=0)
        value = value + pltpu.roll(value, 64, 1)
        value = value + pltpu.roll(value, 16, 1)
        return value + pltpu.roll(value, 32, 1)

    first = over_groups(weighted)
    second = over_groups(squared)
    count = 64.0 - outside
    mean = (first - weighted[0]) / count
    variance = (second - squared[0]) / count - mean * mean
    score = (conf[0] - mean) * lax.rsqrt(jnp.maximum(variance, 0.0) + VAR_FLOOR)
    rows = jnp.broadcast_to(score, (8, 128))
    placed = rows
    for j in range(1, 4):
        placed = jnp.where(line == j, pltpu.roll(rows, 128 - 16 * j, 1), placed)
    out_ref[...] = placed[0:4, 0:16]

    for side in range(2):
        for k in range(4):
            for n in VIA_Z if k == 3 else range(CUTS):
                z_copy(k, side == 0, n).wait_send()
        for m in range(4):
            for n in range(CUTS):
                if m < 3 or n not in VIA_Z:
                    y_copy(m, side == 0, n).wait_send()
        for g in range(8):
            for n in range(CUTS):
                c_copy(g, side, n).wait_send()
    for i in range(PARTS):
        hz_copy(i).wait_send()
        hy_copy(i).wait_send()
        for part in range(2):
            for dx in (1, 3, 2):
                hx_copy(part, i, dx).wait_send()
    all_plane.wait_send()
    all_shadows.wait_send()


def per_device(hidden, targets, membership, unembedding):
    shadow_count, token_count, width = hidden.shape
    dma = pltpu.SemaphoreType.DMA
    return pl.pallas_call(
        kernel,
        out_shape=pltpu.VMEM((4, 16), jnp.float32),
        in_specs=[pl.BlockSpec(memory_space=pltpu.HBM)] * 4,
        out_specs=pl.BlockSpec(memory_space=pltpu.VMEM),
        scratch_shapes=[
            pltpu.VMEM((1, 128), jnp.int32),
            pltpu.SMEM((4, 4), jnp.int32),
            pltpu.SMEM((32,), jnp.int32),
            pltpu.VMEM((2, 512, width), jnp.bfloat16),
            pltpu.VMEM((32, HALF, width), jnp.bfloat16),
            pltpu.VMEM((4, 8 * HALF, NT), jnp.float32),
            pltpu.VMEM((2, 8, 512), jnp.float32),
            pltpu.VMEM((2, 8, 512), jnp.float32),
            pltpu.VMEM((2, 8, 512), jnp.float32),
            pltpu.VMEM((8, NT), jnp.int32),
            pltpu.VMEM((8, 2, 1, 128), jnp.float32),
            pltpu.VMEM((8, 2, 1, 128), jnp.float32),
            pltpu.VMEM((3, 1, 128), jnp.float32),
            pltpu.VMEM((32, 3, 1, 128), jnp.float32),
            dma((4,)), dma((2, 4, CUTS)), dma((2, 4, CUTS)), dma((2, 4, CUTS)), dma((2, 4, CUTS)),
            dma((2, 8, CUTS)), dma((2, 8, CUTS)),
            dma((PARTS,)), dma((PARTS,)), dma((PARTS,)), dma((PARTS,)),
            dma((2, PARTS, 3)), dma((2, PARTS, 3)), dma((2,)), dma((2,)),
        ],
        compiler_params=pltpu.CompilerParams(
            collective_id=0, has_side_effects=True, vmem_limit_bytes=60 * 2**20
        ),
        name="score_kernel",
    )(*(pltpu.with_memory_space_constraint(a, pltpu.HBM) for a in (
        hidden.reshape(shadow_count * token_count, width),
        unembedding.reshape(2, HALF, width),
        targets.reshape(1, token_count), membership,
    )))


def solution(mesh):
    return jax.shard_map(
        per_device,
        mesh=mesh,
        in_specs=(P("shadow", None, None), P(), P("shadow", None), P(("shadow", "vocab"), None)),
        out_specs=P("shadow", "vocab"),
        check_vma=False,
    )
```

```python
import functools

import jax
import jax.numpy as jnp
from jax import lax
from jax.experimental import pallas as pl
from jax.experimental.pallas import tpu as pltpu
from jax.sharding import PartitionSpec as P

NEG_FILL = -1e30
VAR_FLOOR = 0.5
MESH = pl.DeviceIdType.MESH
NZ = 8
HALF = 64
NT = 256
PARTS = 4
ROWS = 64 // PARTS
CUTS = 2
CUT = HALF // CUTS
VIA_Z = (1,)
FIRST_X = (1, 3, 2)

GROUPS = (
    ((0, 0, 0), (0, 0, 1)),
    ((0, -1, 0), (0, 1, 1)),
    ((-1, 0, 0), (1, 0, 1)),
    ((-1, -1, 0), (1, 1, 1)),
    ((-1, 0, 1), (1, 0, 0)),
    ((1, -1, 0), (-1, 1, 1)),
    ((-2, 0, 0), (2, 0, 1)),
    ((-2, -1, 0), (2, 1, 1)),
)


def kernel(
    hidden_hbm, head_hbm, targets_hbm, member_hbm, out_ref,
    targets_ref, member_ref, bases, hid, head, logits, high, total, hit_logit, tg,
    msg, got1, msg2, got2,
    local_sem, z_send, z_recv, y_send, y_recv, c_send, c_recv,
    hz_send, hz_recv, hy_send, hy_recv, hx_send, hx_recv, tail_send, tail_recv,
):
    shadow = lax.axis_index("shadow")
    vocab = lax.axis_index("vocab")
    z = shadow // 4
    y_lo = (shadow // 2) % 2
    core = shadow % 2
    y_hi = vocab // 4
    x = vocab % 4
    y = y_hi * 2 + y_lo

    def device(dz, dy, dx, dcore):
        to_y = (y + dy) % 4
        return (
            (((z + dz) % NZ) * 2 + to_y % 2) * 2 + (core + dcore) % 2,
            (to_y // 2) * 4 + (x + dx) % 4,
        )

    own_head = pltpu.make_async_copy(head_hbm, head.at[pl.ds(0, 2)], local_sem.at[0])
    own_hid = pltpu.make_async_copy(hidden_hbm, hid.at[0], local_sem.at[1])
    own_tg = pltpu.make_async_copy(targets_hbm, targets_ref, local_sem.at[2])
    own_member = pltpu.make_async_copy(member_hbm, member_ref, local_sem.at[3])
    own_head.start()
    own_hid.start()
    own_tg.start()
    own_member.start()

    barrier = pltpu.get_barrier_semaphore()
    near = ((1, 0, 0, 0), (7, 0, 0, 0), (4, 0, 0, 0), (0, 1, 0, 0), (0, 3, 0, 0), (0, 2, 0, 0), (0, 0, 1, 0), (0, 0, 3, 0), (0, 0, 2, 0), (0, 0, 0, 1))
    for offset in near:
        pl.semaphore_signal(barrier, inc=1, device_id=device(*offset), device_id_type=MESH)

    high[...] = jnp.full_like(high, NEG_FILL)
    total[...] = jnp.zeros_like(total)
    hit_logit[...] = jnp.zeros_like(hit_logit)
    for g in range(8):
        for u in range(4):
            dz, dy, half = GROUPS[g][u % 2]
            at_y = (y + dy + 4) % 4
            block = ((((z + dz + NZ) % NZ) * 2 + at_y % 2) * 2 + (core + u // 2) % 2) * 8 + (at_y // 2) * 4 + x
            bases[4 * g + u] = block * (2 * HALF) + half * HALF
    own_tg.wait()
    own_member.wait()
    wide = jnp.broadcast_to(targets_ref[...], (8, 128))
    tg[:, 0:128] = wide
    tg[:, 128:256] = wide

    def z_copy(k, upward, n):
        rows = pl.ds(n * CUT, CUT)
        side = 0 if upward else 1
        src = (side, 1 - side, 8 + side, 12 + side)[k]
        dst = (8, 16, 24, 28)[k] + side
        return pltpu.make_async_remote_copy(
            src_ref=head.at[src, rows, :], dst_ref=head.at[dst, rows, :],
            send_sem=z_send.at[side, k, n], recv_sem=z_recv.at[side, k, n],
            device_id=device(1 if upward else NZ - 1, 0, 0, 0), device_id_type=MESH,
        )

    def y_copy(m, upward, n):
        rows = pl.ds(n * CUT, CUT)
        side = 0 if upward else 1
        src = ((0, 8, 17, 24) if upward else (1, 9, 16, 25))[m]
        return pltpu.make_async_remote_copy(
            src_ref=head.at[src, rows, :], dst_ref=head.at[8 * m + 4 + side, rows, :],
            send_sem=y_send.at[side, m, n], recv_sem=y_recv.at[side, m, n],
            device_id=device(0, 1 if upward else 3, 0, 0), device_id_type=MESH,
        )

    def c_copy(g, side, n):
        rows = pl.ds(n * CUT, CUT)
        return pltpu.make_async_remote_copy(
            src_ref=head.at[4 * g + side, rows, :], dst_ref=head.at[4 * g + 2 + side, rows, :],
            send_sem=c_send.at[side, g, n], recv_sem=c_recv.at[side, g, n],
            device_id=device(0, 0, 0, 1), device_id_type=MESH,
        )

    def hz_copy(i):
        rows = pl.ds(pl.multiple_of(vocab * 64 + i * ROWS, ROWS), ROWS)
        return pltpu.make_async_remote_copy(
            src_ref=hid.at[0, rows, :], dst_ref=hid.at[1, rows, :],
            send_sem=hz_send.at[i], recv_sem=hz_recv.at[i],
            device_id=device(4, 0, 0, 0), device_id_type=MESH,
        )

    def hy_copy(i):
        rows = pl.ds(pl.multiple_of(vocab * 64 + i * ROWS, ROWS), ROWS)
        return pltpu.make_async_remote_copy(
            src_ref=hid.at[1, rows, :], dst_ref=hid.at[1, rows, :],
            send_sem=hy_send.at[i], recv_sem=hy_recv.at[i],
            device_id=device(0, 2, 0, 0), device_id_type=MESH,
        )

    def hx_copy(part, i, dx):
        to_x, owner = dx, x
        if part == 1 and dx == 2:
            to_x = 1 if i % 2 == 0 else 3
            owner = (x + 4 - to_x) % 4
        share = ((y_hi + part) % 2) * 4 + owner
        rows = pl.ds(pl.multiple_of(share * 64 + i * ROWS, ROWS), ROWS)
        return pltpu.make_async_remote_copy(
            src_ref=hid.at[1, rows, :], dst_ref=hid.at[1, rows, :],
            send_sem=hx_send.at[part, i, dx - 1], recv_sem=hx_recv.at[part, i, dx - 1],
            device_id=device(0, 0, to_x, 0), device_id_type=MESH,
        )

    def columns(tile):
        return pl.ds(pl.multiple_of(tile * NT, NT), NT)

    def product(g, count, piece, tile, buf):
        lhs = head[4 * g:4 * (g + count)].reshape(4 * count * HALF, head.shape[2])
        rhs = hid[piece, columns(tile), :]
        logits[buf, 0:4 * count * HALF] = lax.dot_general(
            lhs, rhs, (((1,), (1,)), ((), ())), preferred_element_type=jnp.float32
        )

    def fold(first, count, piece, tile, buf):
        for g in range(first, first + count):
            fold_group(g, (g - first) * 4, piece, columns(tile), buf)

    def fold_group(g, at, piece, cols, buf):
        ids = lax.broadcasted_iota(jnp.int32, (8, 8, NT), 1) + 8 * lax.broadcasted_iota(
            jnp.int32, (8, 8, NT), 0
        )
        found = hit_logit[piece, :, cols]
        others = []
        old = high[piece, :, cols]
        new = old
        for u in range(4):
            v = logits[buf, (at + u) * HALF:(at + u + 1) * HALF, :].reshape(8, 8, NT)
            hit = (tg[...] - bases[4 * g + u])[None] == ids
            found = found + jnp.sum(jnp.where(hit, v, 0.0), axis=0)
            v = jnp.where(hit, 2.0 * NEG_FILL, v)
            new = jnp.maximum(new, jnp.max(v, axis=0))
            others.append(v)
        fresh = total[piece, :, cols] * jnp.exp(old - new)
        for v in others:
            fresh = fresh + jnp.sum(jnp.exp(v - new[None]), axis=0)
        high[piece, :, cols] = new
        total[piece, :, cols] = fresh
        hit_logit[piece, :, cols] = found

    def multiply(*tiles):
        for i, tile in enumerate(tiles):
            product(*tile, i % 4)
            if i:
                fold(*tiles[i - 1], (i - 1) % 4)
        fold(*tiles[-1], (len(tiles) - 1) % 4)

    own_tile, far_tile = y_hi, 1 - y_hi

    def on_z(k, n):
        for side in range(2):
            upward = side == 0
            z_copy(k, upward, n).wait_recv()
            if k == 0:
                z_copy(2, upward, n).start()
            if k < 2 or (k == 2 and n not in VIA_Z):
                y_copy(k + 1, upward == (k != 1), n).start()
            c_copy(7 if k == 3 else 2 * k + 2, side, n).start()

    def on_y(m, n):
        for side in range(2):
            y_copy(m, side == 0, n).wait_recv()
            if m == 1 and n in VIA_Z:
                z_copy(3, side == 0, n).start()
            c_copy(2 * m + 1, side, n).start()

    def on_c(g):
        for side in range(2):
            for n in range(CUTS):
                c_copy(g, side, n).wait_recv()

    def on_hz(i):
        hz_copy(i).wait_recv()
        hy_copy(i).start()
        for dx in FIRST_X:
            hx_copy(0, i, dx).start()

    def on_hy(i):
        hy_copy(i).wait_recv()
        for dx in (1, 3):
            hx_copy(1, i, dx).start()

    def on_hx(i):
        for dx in (1, 3):
            hx_copy(1, i, dx).wait_recv()
            if (dx == 1) == (i % 2 == 0):
                hx_copy(1, i, 2).start()

    def on_hend(part):
        for i in range(PARTS):
            for dx in (1, 3, 2) if part == 0 else (2,):
                hx_copy(part, i, dx).wait_recv()

    pl.semaphore_wait(barrier, len(near))
    own_head.wait()
    for n in range(CUTS):
        c_copy(0, 0, n).start()
        c_copy(0, 1, n).start()
    for n in range(CUTS):
        y_copy(0, True, n).start()
        y_copy(0, False, n).start()
    own_hid.wait()
    hz_copy(0).start()
    hz_copy(1).start()
    hz_copy(2).start()
    hz_copy(3).start()
    z_copy(0, True, 0).start()
    z_copy(0, False, 0).start()
    z_copy(0, True, 1).start()
    z_copy(0, False, 1).start()
    z_copy(1, True, 0).start()
    z_copy(1, False, 0).start()
    z_copy(1, True, 1).start()
    z_copy(1, False, 1).start()
    on_c(0)
    multiply((0, 1, 0, 0), (0, 1, 0, 1))
    on_y(0, 0)
    on_hz(0)
    on_y(0, 1)
    on_c(1)
    multiply((1, 1, 0, 0), (1, 1, 0, 1))
    on_hz(1)
    on_hz(2)
    on_hz(3)
    on_hy(0)
    on_hy(1)
    on_z(0, 0)
    on_hy(2)
    on_z(0, 1)
    on_hy(3)
    on_c(2)
    multiply((2, 1, 0, 0), (2, 1, 0, 1))
    on_y(1, 0)
    on_z(1, 0)
    on_hx(0)
    on_hx(1)
    on_hend(0)
    multiply((0, 1, 1, own_tile), (1, 1, 1, own_tile))
    on_y(1, 1)
    on_z(1, 1)
    on_hx(2)
    on_hx(3)
    on_c(3)
    multiply((2, 1, 1, own_tile), (3, 1, 0, 0), (3, 1, 0, 1), (3, 1, 1, own_tile))
    on_y(2, 0)
    on_z(2, 0)
    on_c(4)
    multiply((4, 1, 0, 0), (4, 1, 0, 1), (4, 1, 1, own_tile))
    on_hend(1)
    multiply((0, 1, 1, far_tile))
    on_y(2, 1)
    on_z(2, 1)
    multiply((1, 1, 1, far_tile), (2, 1, 1, far_tile), (3, 1, 1, far_tile), (4, 1, 1, far_tile))
    on_c(5)
    multiply((5, 1, 0, 0), (5, 1, 0, 1), (5, 1, 1, own_tile), (5, 1, 1, far_tile))
    on_y(3, 0)
    on_z(3, 1)
    on_c(6)
    multiply((6, 1, 0, 0), (6, 1, 0, 1), (6, 1, 1, own_tile), (6, 1, 1, far_tile))
    on_c(7)
    multiply((7, 1, 0, 0), (7, 1, 0, 1), (7, 1, 1, own_tile), (7, 1, 1, far_tile))

    lane = lax.broadcasted_iota(jnp.int32, (8, 128), 1)
    line = lax.broadcasted_iota(jnp.int32, (8, 128), 0)
    lse_tile = jnp.zeros((8, 128), jnp.float32)
    target_tile = jnp.zeros((8, 128), jnp.float32)
    for piece in range(2):
        peak = jnp.max(high[piece], axis=0, keepdims=True)
        summed = jnp.sum(total[piece] * jnp.exp(high[piece] - peak), axis=0, keepdims=True)
        partial = peak + jnp.log(summed)
        at_target = jnp.sum(hit_logit[piece], axis=0, keepdims=True)
        for j in range(4):
            part = slice(j * 128, (j + 1) * 128)
            here = line == piece * 4 + j
            lse_tile = jnp.where(here, jnp.broadcast_to(partial[:, part], (8, 128)), lse_tile)
            target_tile = jnp.where(here, jnp.broadcast_to(at_target[:, part], (8, 128)), target_tile)

    def swap_groups(tile):
        swapped = tile
        for d in range(1, 8):
            moved = pltpu.roll(pltpu.roll(tile, d, 0), 128 - 16 * d, 1)
            swapped = jnp.where((line - lane // 16 + 8) % 8 == d, moved, swapped)
        return swapped

    lse_tile = swap_groups(lse_tile)
    target_tile = swap_groups(target_tile)
    for r in range(8):
        msg[r, 0] = lse_tile[r:r + 1, :]
        msg[r, 1] = target_tile[r:r + 1, :]

    def to_plane(k):
        to = (vocab + k) % 8
        pltpu.make_async_remote_copy(
            src_ref=msg.at[to], dst_ref=got1.at[7 - k],
            send_sem=tail_send.at[0], recv_sem=tail_recv.at[0],
            device_id=(shadow, to), device_id_type=MESH,
        ).start()

    for k in (6, 2, 5, 7, 4, 1, 3):
        to_plane(k)
    got1[7] = msg[vocab]
    all_plane = pltpu.make_async_remote_copy(
        src_ref=msg.at[0:7], dst_ref=got1.at[0:7],
        send_sem=tail_send.at[0], recv_sem=tail_recv.at[0],
        device_id=device(0, 0, 0, 1), device_id_type=MESH,
    )
    lane = lax.broadcasted_iota(jnp.int32, (1, 128), 1)
    group = (lane % 64) // 16
    outside = jnp.zeros((1, 128), jnp.float32)
    for j in range(4):
        free = (1 - member_ref[j, vocab // 2]).astype(jnp.float32)
        outside = jnp.where(group == j, free, outside)
    msg2[2] = outside
    all_plane.wait_recv()

    pieces = got1[:, 0]
    top = jnp.max(pieces, axis=0)
    msg2[0] = top + jnp.log(jnp.sum(jnp.exp(pieces - top[None]), axis=0))
    msg2[1] = jnp.sum(got1[:, 1], axis=0)

    def to_shadows(k):
        dz, dy, dcore = k // 4, (k // 2) % 2, k % 2
        to = (((z + dz) % NZ) * 2 + (y_lo + dy) % 2) * 2 + (core + dcore) % 2
        pltpu.make_async_remote_copy(
            src_ref=msg2, dst_ref=got2.at[((NZ - dz) % NZ) * 4 + k % 4],
            send_sem=tail_send.at[1], recv_sem=tail_recv.at[1],
            device_id=(to, vocab), device_id_type=MESH,
        ).start()

    for dz in (4, 3, 5, 2, 6, 1, 7, 0):
        for k in range(max(4 * dz, 1), 4 * dz + 4):
            to_shadows(k)
    got2[0] = msg2[...]
    all_shadows = pltpu.make_async_remote_copy(
        src_ref=got2.at[1:32], dst_ref=got2.at[1:32],
        send_sem=tail_send.at[1], recv_sem=tail_recv.at[1],
        device_id=device(0, 0, 0, 1), device_id_type=MESH,
    )
    all_shadows.wait_recv()

    def both_planes(row):
        there = jnp.concatenate([got2[16:32, row], got2[0:16, row]], axis=0)
        return got2[:, row], pltpu.roll(there, 64, 2)

    here, there = both_planes(0)
    top = jnp.maximum(here, there)
    lse = top + jnp.log(jnp.exp(here - top) + jnp.exp(there - top))
    here, there = both_planes(1)
    conf = (here + there) - lse
    weighted = jnp.where(lane < 64, got2[:, 2] * conf, 0.0)
    squared = weighted * conf

    def over_groups(value):
        value = jnp.sum(value, axis=0)
        value = value + pltpu.roll(value, 64, 1)
        value = value + pltpu.roll(value, 16, 1)
        return value + pltpu.roll(value, 32, 1)

    first = over_groups(weighted)
    second = over_groups(squared)
    count = 64.0 - outside
    mean = (first - weighted[0]) / count
    variance = (second - squared[0]) / count - mean * mean
    score = (conf[0] - mean) * lax.rsqrt(jnp.maximum(variance, 0.0) + VAR_FLOOR)
    rows = jnp.broadcast_to(score, (8, 128))
    placed = rows
    for j in range(1, 4):
        placed = jnp.where(line == j, pltpu.roll(rows, 128 - 16 * j, 1), placed)
    out_ref[...] = placed[0:4, 0:16]

    for side in range(2):
        for k in range(4):
            for n in VIA_Z if k == 3 else range(CUTS):
                z_copy(k, side == 0, n).wait_send()
        for m in range(4):
            for n in range(CUTS):
                if m < 3 or n not in VIA_Z:
                    y_copy(m, side == 0, n).wait_send()
        for g in range(8):
            for n in range(CUTS):
                c_copy(g, side, n).wait_send()
    for i in range(PARTS):
        hz_copy(i).wait_send()
        hy_copy(i).wait_send()
        for part in range(2):
            for dx in (1, 3, 2):
                hx_copy(part, i, dx).wait_send()
    all_plane.wait_send()
    all_shadows.wait_send()


def per_device(hidden, targets, membership, unembedding):
    shadow_count, token_count, width = hidden.shape
    dma = pltpu.SemaphoreType.DMA
    return pl.pallas_call(
        kernel,
        out_shape=pltpu.VMEM((4, 16), jnp.float32),
        in_specs=[pl.BlockSpec(memory_space=pltpu.HBM)] * 4,
        out_specs=pl.BlockSpec(memory_space=pltpu.VMEM),
        scratch_shapes=[
            pltpu.VMEM((1, 128), jnp.int32),
            pltpu.SMEM((4, 4), jnp.int32),
            pltpu.SMEM((32,), jnp.int32),
            pltpu.VMEM((2, 512, width), jnp.bfloat16),
            pltpu.VMEM((32, HALF, width), jnp.bfloat16),
            pltpu.VMEM((4, 8 * HALF, NT), jnp.float32),
            pltpu.VMEM((2, 8, 512), jnp.float32),
            pltpu.VMEM((2, 8, 512), jnp.float32),
            pltpu.VMEM((2, 8, 512), jnp.float32),
            pltpu.VMEM((8, NT), jnp.int32),
            pltpu.VMEM((8, 2, 1, 128), jnp.float32),
            pltpu.VMEM((8, 2, 1, 128), jnp.float32),
            pltpu.VMEM((3, 1, 128), jnp.float32),
            pltpu.VMEM((32, 3, 1, 128), jnp.float32),
            dma((4,)), dma((2, 4, CUTS)), dma((2, 4, CUTS)), dma((2, 4, CUTS)), dma((2, 4, CUTS)),
            dma((2, 8, CUTS)), dma((2, 8, CUTS)),
            dma((PARTS,)), dma((PARTS,)), dma((PARTS,)), dma((PARTS,)),
            dma((2, PARTS, 3)), dma((2, PARTS, 3)), dma((2,)), dma((2,)),
        ],
        compiler_params=pltpu.CompilerParams(
            collective_id=0, has_side_effects=True, vmem_limit_bytes=60 * 2**20
        ),
        name="score_kernel",
    )(*(pltpu.with_memory_space_constraint(a, pltpu.HBM) for a in (
        hidden.reshape(shadow_count * token_count, width),
        unembedding.reshape(2, HALF, width),
        targets.reshape(1, token_count), membership,
    )))


def solution(mesh):
    return jax.shard_map(
        per_device,
        mesh=mesh,
        in_specs=(P("shadow", None, None), P(), P("shadow", None), P(("shadow", "vocab"), None)),
        out_specs=P("shadow", "vocab"),
        check_vma=False,
    )
```
